768 devices in a mesh: gx: 12 (over z), gy: 16 (over y_lo, x, core), gz: 4 (over y_hi).
Axes of the slice: x: 4, y: 8 (y_hi: 4, y_lo: 2; y = y_hi * 2 + y_lo), z: 12, core: 2. Of those that a mesh axis runs over, the one named last changes fastest.
Arguments:
- hidden_in: bfloat16 [24576, 4096], P(('gx', 'gy'), 'gz'), may hold values from -40 to 40
- norm_gain: float32 [4096], P('gz'), may hold values from 0.25 to 1.75
- normed_grad: bfloat16 [24576, 4096], P(('gx', 'gy'), 'gz'), may hold values from -64 to 64
- key_grad: bfloat16 [24576, 512], P(('gx', 'gy')), may hold values from -6 to 6
- weight_blocks: bfloat16 [192, 4, 29, 128], P(('gx', 'gy'), 'gz'), may hold values from -0.09375 to 0.09375
- block_count: int32 [4, 192], P('gz'), may hold values from 1 to 29, as said below
Outputs:
- hidden_grad: bfloat16 [24576, 4096], P(('gx', 'gy'), 'gz')
- weight_grad: float32 [192, 4, 29, 128], P(('gx', 'gy'), 'gz')
The draws below stay inside these ranges and needn't reach their ends.
Inputs may be any that keep to these rules, and one draw needn't show every extreme that they name: `block_count`: each row sums to 4096; in each row the owners i * 16 to i * 16 + 15 hold together exactly the blocks i * 342 to min((i + 1) * 342, 4096) - 1, and one of them holds exactly 29 blocks.
All inputs are finite; a program needn't handle non-finite values.
Results may differ from the reference program's by a relative error of at most 0.0029.
Values may be sent and summed in bfloat16 or wider, within the bound.
A program may use at most 32 MiB of HBM per device.

```python
import math
import jax
import jax.numpy as jnp
from jax import lax

D = 4096
KVW = 512
TOK_DEV = 128
OUTER = 12
INNER = 16
OWNERS = 192
TOKENS = 24576
QUARTERS = 4
BLOCKS = 4096
GROUPB = 342
MAXB = 29


def joint_activations(key):
    subkeys = jax.random.split(jax.random.fold_in(key, 7001), 5)
    position = jnp.arange(D, dtype=jnp.float32) / D
    base = jnp.clip(jax.random.normal(subkeys[0], (TOKENS, D), jnp.float32), -4.0, 4.0)
    column = jnp.power(3.0, position) * jnp.exp(jax.random.uniform(subkeys[1], (D,), jnp.float32, math.log(0.6), math.log(1.6)))
    hidden = base * column[None, :]
    coefficient = jax.random.uniform(subkeys[3], (TOKENS, 1), jnp.float32, -1.5, 1.5)
    noise = 0.5 * jnp.clip(jax.random.normal(subkeys[4], (TOKENS, D), jnp.float32), -4.0, 4.0)
    return (hidden, coefficient * hidden + noise)


def draw_hidden_in(key, part):
    hidden, _ = joint_activations(key)
    return hidden.astype(jnp.bfloat16)


def draw_normed_grad(key, part):
    _, cotangent = joint_activations(key)
    return cotangent.astype(jnp.bfloat16)


def draw_block_count(key, part):
    subkeys = jax.random.split(jax.random.fold_in(key, 7002), 2)
    group_ids = jnp.arange(OUTER, dtype=jnp.int32)
    totals = jnp.minimum(GROUPB, BLOCKS - group_ids * GROUPB).astype(jnp.int32)
    totals = jnp.broadcast_to(totals[None, :, None], (QUARTERS, OUTER, 1))
    chosen = jax.random.randint(subkeys[0], (QUARTERS, OUTER, 1), 0, INNER, dtype=jnp.int32)
    member = jnp.arange(INNER, dtype=jnp.int32)[None, None, :]
    is_full = member == chosen
    raw_weight = jax.random.randint(subkeys[1], (QUARTERS, OUTER, INNER), 1, 6, dtype=jnp.int32)
    weights = jnp.where(is_full, 0, raw_weight * raw_weight * raw_weight)
    extra = totals - MAXB - (INNER - 1)
    share = extra * weights // jnp.sum(weights, axis=2, keepdims=True)
    share = jnp.minimum(share, MAXB - 1)
    leftover = extra - jnp.sum(share, axis=2, keepdims=True)
    room = jnp.where(is_full, 0, MAXB - 1 - share)
    before = jnp.cumsum(room, axis=2) - room
    share = share + jnp.clip(leftover - before, 0, room)
    counts = jnp.where(is_full, MAXB, 1 + share)
    return counts.reshape(QUARTERS, OWNERS).astype(jnp.int32)


def block_levels(stream_key, dims, cuts, low, largest):
    factor_of = 1.0
    for dim, blocks in cuts:
        steps = jax.random.uniform(jax.random.fold_in(jax.random.fold_in(stream_key, 6), dim), (blocks,), jnp.float32, low / len(cuts), largest / len(cuts))
        factor_of = factor_of * jnp.repeat(jnp.exp(steps), dims[dim] // blocks).reshape((-1,) + (1,) * (len(dims) - 1 - dim))
    return factor_of


def scatter_about(rng, dims, deviation, most, cuts=(), held_as=jnp.bfloat16):
    loudness = block_levels(rng, dims, cuts, -0.22, 0.18) if cuts else 1.0
    result = jax.random.normal(rng, dims, jnp.float32) * deviation * loudness
    return jnp.minimum(jnp.maximum(result, -most), most).astype(held_as)


def setup_inputs(seed: int = 0) -> dict:
    seeds = jax.random.split(jax.random.key(seed), 7)
    return {
        "hidden_in": draw_hidden_in(jax.random.fold_in(seeds[6], 71), 0),
        "norm_gain": jnp.clip(1.0 + 0.15 * jax.random.normal(seeds[1], (D,), jnp.float32), 0.25, 1.75),
        "normed_grad": draw_normed_grad(jax.random.fold_in(seeds[6], 71), 0),
        "key_grad": scatter_about(seeds[3], (TOKENS, KVW), 1.0, 6.0, ((0, 192),)),
        "weight_blocks": scatter_about(seeds[4], (OWNERS, QUARTERS, MAXB, 128), D ** -0.5, 0.09375, ((0, 192), (1, 4))),
        "block_count": draw_block_count(jax.random.fold_in(seeds[6], 71), 0),
    }


EPS = 1e-06

def block_layout(counts):
    ends = jnp.cumsum(counts).astype(jnp.int32)
    starts = (ends - counts).astype(jnp.int32)
    block_ids = jnp.arange(BLOCKS, dtype=jnp.int32)
    owner = jnp.searchsorted(ends, block_ids, side='right').astype(jnp.int32)
    gather_index = (owner * MAXB + block_ids - starts[owner]).astype(jnp.int32)
    slot_owner = jnp.arange(OWNERS * MAXB, dtype=jnp.int32) // MAXB
    slot_within = jnp.arange(OWNERS * MAXB, dtype=jnp.int32) % MAXB
    valid = slot_within < counts[slot_owner]
    source = jnp.clip(starts[slot_owner] + slot_within, 0, BLOCKS - 1).astype(jnp.int32)
    return (gather_index, source, valid)

def reference(hidden_in, norm_gain, normed_grad, key_grad, weight_blocks, block_count):
    group_rows = D // QUARTERS
    pieces = []
    layouts = []
    for group in range(QUARTERS):
        gather_index, source, valid = block_layout(block_count[group])
        layouts.append((source, valid))
        rows = weight_blocks[:, group].reshape(OWNERS * MAXB, 128)
        pieces.append(rows[gather_index].reshape(group_rows, KVW))
    weight = jnp.concatenate(pieces, axis=0)
    gain = norm_gain.astype(jnp.float32)

    def step(total, items):
        hblock, nblock, kblock = items
        hfloat = hblock.astype(jnp.float32)
        rstd = lax.rsqrt(lax.optimization_barrier(jnp.sum(hfloat * hfloat, axis=1)) / D + EPS)
        normed = (hfloat * rstd[:, None] * gain).astype(jnp.bfloat16)
        total = total + lax.dot_general(normed, kblock, (((0,), (0,)), ((), ())), preferred_element_type=jnp.float32)
        dnorm = nblock.astype(jnp.float32) + lax.dot_general(kblock, weight, (((1,), (1,)), ((), ())), preferred_element_type=jnp.float32)
        proj = lax.optimization_barrier(jnp.sum(gain * dnorm * hfloat, axis=1))
        grad = gain * dnorm * rstd[:, None] - hfloat * (rstd ** 3 * proj / D)[:, None]
        return (total, grad.astype(jnp.bfloat16))
    hsplit = hidden_in.reshape(OWNERS, TOK_DEV, D)
    nsplit = normed_grad.reshape(OWNERS, TOK_DEV, D)
    ksplit = key_grad.reshape(OWNERS, TOK_DEV, KVW)
    dweight, grads = lax.scan(step, jnp.zeros((D, KVW), jnp.float32), (hsplit, nsplit, ksplit))
    outs = []
    for group in range(QUARTERS):
        source, valid = layouts[group]
        flat = dweight[group * group_rows:(group + 1) * group_rows].reshape(BLOCKS, 128)
        padded = jnp.where(valid[:, None], flat[source], jnp.float32(0.0))
        outs.append(padded.reshape(OWNERS, MAXB, 128))
    weight_grad = jnp.stack(outs, axis=1)
    return (grads.reshape(TOKENS, D), weight_grad)
```

```python
import functools

import jax
import jax.numpy as jnp
from jax import lax
from jax.experimental import pallas as pl
from jax.experimental.pallas import tpu as pltpu
from jax.sharding import PartitionSpec as P

EPS = 1e-06
LANES = 128
CORES = 2
F32 = jnp.float32
BF16 = jnp.bfloat16
MESH = pl.DeviceIdType.MESH
BATCHES = 4


def round_up(value, step):
    return (value + step - 1) // step * step


def iota(shape, dim):
    return lax.broadcasted_iota(jnp.int32, shape, dim)


def nt_dot(a, b):
    return lax.dot_general(a, b, (((1,), (1,)), ((), ())), preferred_element_type=F32)


def as_column(row):
    return jnp.transpose(jnp.broadcast_to(row, (LANES, LANES)))


def lane_groups(rows):
    return [slice(g * LANES, (g + 1) * LANES) for g in range(rows // LANES)]


def kernel(
    cfg,
    h_hbm, gain_hbm, ng_hbm, kg_hbm, wb_hbm, cnt_hbm,
    hg_hbm, wg_ref,
    h2, gainv, ngv, kg2, wbv, cntv,
    sq, pj, rs, nrm, onehot, onehot_t, jcol,
    gathered, send, recv, zsend, zrecv, wfull, p_own, p_send, p_recv, hgv,
    local_sem, sq_s, sq_r, sib_s, sib_r, c1_s, c1_r, b_s, b_r, c2_s, c2_r, pj_s, pj_r, z_s, z_r,
):
    outer, inner, quarters, chips = cfg["outer"], cfg["inner"], cfg["quarters"], cfg["chips"]
    slots, most, group_blocks, blocks = cfg["slots"], cfg["most"], cfg["group_blocks"], cfg["blocks"]
    rows, width, pieces, model_width = cfg["rows"], cfg["width"], cfg["pieces"], cfg["model_width"]
    lane_window, row_window, padded_outer = cfg["lane_window"], cfg["row_window"], cfg["padded_outer"]
    per_group = chips * slots
    owners = outer * inner
    slot_bits = slots.bit_length() - 1
    inner_bits = inner.bit_length() - 1
    piece_bits = pieces.bit_length() - 1

    x = lax.axis_index("gx")
    y = lax.axis_index("gy")
    q = lax.axis_index("gz")
    core = lax.rem(y, CORES)
    chip = y // CORES
    other = 1 - core
    own_rows = pl.ds(pl.multiple_of(core * LANES, LANES), LANES)
    other_rows = pl.ds(pl.multiple_of(other * LANES, LANES), LANES)

    def at(gx, gchip, gcore, gz):
        return (gx, gchip * CORES + gcore, gz)

    z_peers = [(k, lax.rem(x + k, outer)) for k in range(1, outer)]
    z_peers.sort(key=lambda p: -min(p[0], outer - p[0]))
    chip_peers = [(k, lax.rem(chip + k, chips)) for k in range(1, chips)]
    gz_peers = [
        (dc * quarters + dq - 1, lax.rem(core + dc, CORES), lax.rem(q + dq, quarters))
        for dc in range(CORES)
        for dq in range(quarters)
        if dc or dq
    ]

    loads = [
        pltpu.make_async_copy(h_hbm, h2.at[core], local_sem.at[0]),
        pltpu.make_async_copy(cnt_hbm, cntv, local_sem.at[1]),
        pltpu.make_async_copy(wb_hbm, wbv, local_sem.at[2]),
        pltpu.make_async_copy(kg_hbm, kg2.at[own_rows], local_sem.at[3]),
        pltpu.make_async_copy(gain_hbm, gainv, local_sem.at[4]),
        pltpu.make_async_copy(ng_hbm, ngv, local_sem.at[5]),
    ]
    for copy in loads:
        copy.start()
    barrier = pltpu.get_barrier_semaphore()
    peers = [at(zx, chip, core, q) for _, zx in z_peers]
    peers += [at(x, other_chip, core, q) for _, other_chip in chip_peers]
    peers += [at(x, chip, gcore, gq) for _, gcore, gq in gz_peers]
    for peer in peers:
        pl.semaphore_signal(barrier, inc=1, device_id=peer, device_id_type=MESH)

    groups = lane_groups(rows)

    loads[0].wait()
    partial = jnp.zeros((LANES, LANES), F32)
    for g in groups:
        piece = h2[core, :, g].astype(F32)
        partial = partial + piece * piece
    row = jnp.sum(jnp.transpose(partial), axis=0, keepdims=True)
    sq[core, q] = jnp.broadcast_to(row, (8, LANES))

    loads[2].wait()
    own_blocks = jnp.concatenate(
        [wbv[0, 0].astype(F32), jnp.zeros((slots - most, LANES), F32)], axis=0
    )
    gathered[chip, x] = own_blocks.astype(BF16)
    loads[3].wait()

    pl.semaphore_wait(barrier, len(peers))

    sends = []

    def push(src, dst, send_sem, recv_sem, peer):
        copy = pltpu.make_async_remote_copy(
            src_ref=src, dst_ref=dst, send_sem=send_sem, recv_sem=recv_sem,
            device_id=peer, device_id_type=MESH,
        )
        copy.start()
        sends.append(copy)
        return copy

    sq_copies = [
        push(sq.at[core, q], sq.at[core, q], sq_s.at[m], sq_r.at[m], at(x, chip, gcore, gq))
        for m, gcore, gq in gz_peers
    ]
    c1_copies = [
        push(gathered.at[chip, x], gathered.at[chip, x], c1_s.at[k - 1], c1_r.at[k - 1], at(zx, chip, core, q))
        for k, zx in z_peers
    ]
    sibling = at(x, chip, other, q)
    sib_copies = [
        push(kg2.at[own_rows], kg2.at[own_rows], sib_s.at[0], sib_r.at[0], sibling),
        push(h2.at[core], h2.at[core], sib_s.at[1], sib_r.at[1], sibling),
    ]

    loads[1].wait()
    loads[4].wait()
    counts = cntv[...].astype(F32)
    owner_of = iota((padded_outer, owners), 1)
    of_group = (owner_of >> inner_bits) == iota((padded_outer, owners), 0)
    by_group = jnp.where(of_group, jnp.broadcast_to(counts, (padded_outer, owners)), 0.0).astype(BF16)

    def placed(shape, slot_dim, owner_dim):
        slot = iota(shape, slot_dim)
        holder = (slot >> slot_bits) * CORES + core
        within = iota(shape, owner_dim) & (inner - 1)
        before = jnp.where(within < holder, 1.0, 0.0).astype(BF16)
        mine = jnp.where(within == holder, 1.0, 0.0).astype(BF16)
        return before, mine

    before, mine = placed((per_group, owners), 0, 1)
    start_c = nt_dot(before, by_group).astype(jnp.int32)
    count_c = nt_dot(mine, by_group).astype(jnp.int32)
    within_c = iota((per_group, padded_outer), 0) & (slots - 1)
    block_c = start_c + within_c + group_blocks * iota((per_group, padded_outer), 1)
    block_c = jnp.where(within_c < count_c, block_c, -pieces)
    row_c = block_c >> piece_bits
    jcol[...] = block_c & (pieces - 1)
    start_r = nt_dot(by_group, before).astype(jnp.int32)
    count_r = nt_dot(by_group, mine).astype(jnp.int32)
    within_r = iota((padded_outer, per_group), 1) & (slots - 1)
    block_r = start_r + within_r + group_blocks * iota((padded_outer, per_group), 0)
    block_r = jnp.where(within_r < count_r, block_r, -pieces)
    row_r = block_r >> piece_bits

    def windows(z):
        first = group_blocks * z // pieces
        return (
            min(first // LANES * LANES, rows - lane_window),
            min(first // 8 * 8, rows - row_window),
        )

    for z in range(outer):
        lane0, row0 = windows(z)
        hit = row_c[:, z : z + 1] == lane0 + iota((per_group, lane_window), 1)
        onehot[z] = jnp.where(hit, 1.0, 0.0).astype(BF16)
        hit = row_r[z : z + 1, :] == row0 + iota((row_window, per_group), 0)
        onehot_t[z] = jnp.where(hit, 1.0, 0.0).astype(BF16)
    wfull[...] = jnp.zeros_like(wfull)

    for copy in sq_copies:
        copy.wait_recv()
    for copy in sib_copies:
        copy.wait_recv()
    for c in range(CORES):
        total = sq[c, 0, 0:1]
        for other_q in range(1, quarters):
            total = total + sq[c, other_q, 0:1]
        rs[c] = as_column(lax.rsqrt(total / model_width + EPS))
        for g in groups:
            scaled = h2[c, :, g].astype(F32) * rs[c] * gainv[:, g]
            nrm[c * LANES : (c + 1) * LANES, g] = scaled.astype(BF16)

    step = outer // BATCHES
    b_copies = []
    for batch in range(BATCHES):
        for z in range(batch * step, (batch + 1) * step):
            lane0, _ = windows(z)
            picked = nt_dot(onehot[z], nrm[:, lane0 : lane0 + lane_window]).astype(BF16)
            product = jnp.dot(picked, kg2[...], preferred_element_type=F32)
            piece_of = jcol[:, z : z + 1]
            value = product[:, :LANES]
            for j in range(1, pieces):
                value = jnp.where(piece_of == j, product[:, j * LANES : (j + 1) * LANES], value)
            send[:, z] = value.astype(BF16).reshape(chips, slots, LANES)
        span = pl.ds(batch * step, step)
        b_copies.append([
            push(
                send.at[to, span], recv.at[k - 1, span], b_s.at[k - 1, batch], b_r.at[k - 1, batch],
                at(x, to, core, q),
            )
            for k, to in chip_peers
        ])

    for copy in c1_copies:
        copy.wait_recv()
    c2_copies = [
        push(gathered.at[chip], gathered.at[chip], c2_s.at[k - 1], c2_r.at[k - 1], at(x, to, core, q))
        for k, to in chip_peers
    ]

    for batch in range(BATCHES):
        for copy in b_copies[batch]:
            copy.wait_recv()
        for z in range(batch * step, (batch + 1) * step):
            total = send[chip, z].astype(F32)
            for k in range(1, chips):
                total = total + recv[k - 1, z].astype(F32)
            zsend[z] = total
    zz_copies = [
        push(zsend.at[zx], zrecv.at[k - 1], z_s.at[k - 1], z_r.at[k - 1], at(zx, chip, core, q))
        for k, zx in z_peers
    ]

    for copy in c2_copies:
        copy.wait_recv()
    for z in range(outer):
        _, row0 = windows(z)
        values = gathered[:, z].reshape(per_group, LANES)
        piece_of = jcol[:, z : z + 1]
        spread = jnp.concatenate(
            [jnp.where(piece_of == j, values, jnp.zeros_like(values)) for j in range(pieces)], axis=1
        )
        wfull[row0 : row0 + row_window, :] += jnp.dot(
            onehot_t[z], spread, preferred_element_type=F32
        )
    weight = wfull[...].astype(BF16)
    p_send[...] = nt_dot(kg2[other_rows], weight)
    p_copy = push(p_send, p_recv, sib_s.at[2], sib_r.at[2], sibling)
    p_own[...] = nt_dot(kg2[own_rows], weight)

    loads[5].wait()
    p_copy.wait_recv()
    partial = jnp.zeros((LANES, LANES), F32)
    for g in groups:
        dnorm = ngv[:, g].astype(F32) + (p_own[:, g] + p_recv[:, g])
        gained = gainv[:, g] * dnorm
        p_own[:, g] = gained
        partial = partial + gained * h2[core, :, g].astype(F32)
    row = jnp.sum(jnp.transpose(partial), axis=0, keepdims=True)
    pj[q] = jnp.broadcast_to(row, (8, LANES))
    pj_copies = [
        push(pj.at[q], pj.at[q], pj_s.at[dq - 1], pj_r.at[dq - 1], at(x, chip, core, lax.rem(q + dq, quarters)))
        for dq in range(1, quarters)
    ]
    for copy in pj_copies:
        copy.wait_recv()
    proj = pj[0, 0:1]
    for other_q in range(1, quarters):
        proj = proj + pj[other_q, 0:1]
    rstd = rs[core]
    coefficient = rstd * rstd * rstd * as_column(proj) / model_width
    for g in groups:
        grad = p_own[:, g] * rstd - h2[core, :, g].astype(F32) * coefficient
        hgv[:, g] = grad.astype(BF16)
    store = pltpu.make_async_copy(hgv, hg_hbm, local_sem.at[6])
    store.start()

    for copy in zz_copies:
        copy.wait_recv()
    total = zsend[x]
    for k in range(1, outer):
        total = total + zrecv[k - 1]
    wg_ref[0, 0] = total[:most]
    store.wait()
    for copy in sends:
        copy.wait_send()


def shards(hidden_in, norm_gain, normed_grad, key_grad, weight_blocks, block_count):
    outer, inner, quarters = lax.axis_size("gx"), lax.axis_size("gy"), lax.axis_size("gz")
    tokens, rows = hidden_in.shape
    width = key_grad.shape[1]
    most = weight_blocks.shape[2]
    blocks = rows * width // LANES
    pieces = width // LANES
    group_blocks = (blocks + outer - 1) // outer
    slots = round_up(most, 32)
    chips = inner // CORES
    per_group = chips * slots
    padded_outer = round_up(outer, 16)
    span = (group_blocks + pieces - 1) // pieces + 1
    cfg = dict(
        outer=outer, inner=inner, quarters=quarters, chips=chips, slots=slots, most=most,
        group_blocks=group_blocks, blocks=blocks, rows=rows, width=width, pieces=pieces,
        model_width=rows * quarters, padded_outer=padded_outer,
        lane_window=min(rows, round_up(span + LANES - 1, LANES)),
        row_window=min(rows, round_up(span + 7, 8)),
    )
    vmem = pltpu.VMEM
    dma = pltpu.SemaphoreType.DMA
    hg, wg = pl.pallas_call(
        functools.partial(kernel, cfg),
        out_shape=(
            jax.ShapeDtypeStruct((tokens, rows), BF16),
            jax.ShapeDtypeStruct(weight_blocks.shape, F32),
        ),
        in_specs=[pl.BlockSpec(memory_space=pl.ANY)] * 6,
        out_specs=(pl.BlockSpec(memory_space=pl.ANY), pl.BlockSpec(memory_space=pltpu.VMEM)),
        scratch_shapes=[
            vmem((CORES, tokens, rows), BF16),
            vmem((1, rows), F32),
            vmem((tokens, rows), BF16),
            vmem((CORES * tokens, width), BF16),
            vmem(weight_blocks.shape, BF16),
            vmem(block_count.shape, jnp.int32),
            vmem((CORES, quarters, 8, LANES), F32),
            vmem((quarters, 8, LANES), F32),
            vmem((CORES, LANES, LANES), F32),
            vmem((CORES * tokens, rows), BF16),
            vmem((outer, per_group, cfg["lane_window"]), BF16),
            vmem((outer, cfg["row_window"], per_group), BF16),
            vmem((per_group, padded_outer), jnp.int32),
            vmem((chips, outer, slots, LANES), BF16),
            vmem((chips, outer, slots, LANES), BF16),
            vmem((chips - 1, outer, slots, LANES), BF16),
            vmem((outer, slots, LANES), F32),
            vmem((outer - 1, slots, LANES), F32),
            vmem((rows, width), F32),
            vmem((tokens, rows), F32),
            vmem((tokens, rows), F32),
            vmem((tokens, rows), F32),
            vmem((tokens, rows), BF16),
            dma((7,)),
            dma((CORES * quarters - 1,)), dma((CORES * quarters - 1,)),
            dma((3,)), dma((3,)),
            dma((outer - 1,)), dma((outer - 1,)),
            dma((chips - 1, BATCHES)), dma((chips - 1, BATCHES)),
            dma((chips - 1,)), dma((chips - 1,)),
            dma((quarters - 1,)), dma((quarters - 1,)),
            dma((outer - 1,)), dma((outer - 1,)),
        ],
        compiler_params=pltpu.CompilerParams(
            collective_id=0, has_side_effects=True, vmem_limit_bytes=48 * 1024 * 1024
        ),
        name="key_projection_backward",
    )(hidden_in, norm_gain.reshape(1, rows), normed_grad, key_grad, weight_blocks, block_count)
    return hg, wg


def solution(mesh):
    placed = (
        P(("gx", "gy"), "gz"),
        P("gz"),
        P(("gx", "gy"), "gz"),
        P(("gx", "gy"), None),
        P(("gx", "gy"), "gz", None, None),
        P("gz", None),
    )
    return jax.shard_map(
        shards,
        mesh=mesh,
        in_specs=placed,
        out_specs=(P(("gx", "gy"), "gz"), P(("gx", "gy"), "gz", None, None)),
        check_vma=False,
    )
```

```python
import functools

import jax
import jax.numpy as jnp
from jax import lax
from jax.experimental import pallas as pl
from jax.experimental.pallas import tpu as pltpu
from jax.sharding import PartitionSpec as P

EPS = 1e-06
LANES = 128
CORES = 2
F32 = jnp.float32
BF16 = jnp.bfloat16
MESH = pl.DeviceIdType.MESH
BATCHES = 4


def round_up(value, step):
    return (value + step - 1) // step * step


def iota(shape, dim):
    return lax.broadcasted_iota(jnp.int32, shape, dim)


def nt_dot(a, b):
    return lax.dot_general(a, b, (((1,), (1,)), ((), ())), preferred_element_type=F32)


def as_column(row):
    return jnp.transpose(jnp.broadcast_to(row, (LANES, LANES)))


def lane_groups(rows):
    return [slice(g * LANES, (g + 1) * LANES) for g in range(rows // LANES)]


def kernel(
    cfg,
    h_hbm, gain_hbm, ng_hbm, kg_hbm, wb_hbm, cnt_hbm,
    hg_ref, wg_ref,
    h2, gainv, ngv, kg2, wbv, cntv,
    sq, pj, rs, nrm, onehot, onehot_t, jcol,
    gathered, kept, y_send, y_recv, x_send, x_recv, zsend, zrecv, wfull, product, p_recv,
    local_sem, sq_s, sq_r, sib_s, sib_r, c1_s, c1_r, by_s, by_r, bx_s, bx_r, c2_s, c2_r, pj_s, pj_r, z_s, z_r,
):
    outer, inner, quarters, chips = cfg["outer"], cfg["inner"], cfg["quarters"], cfg["chips"]
    slots, most, group_blocks, blocks = cfg["slots"], cfg["most"], cfg["group_blocks"], cfg["blocks"]
    rows, width, pieces, model_width = cfg["rows"], cfg["width"], cfg["pieces"], cfg["model_width"]
    lane_window, row_window, padded_outer = cfg["lane_window"], cfg["row_window"], cfg["padded_outer"]
    per_group = chips * slots
    owners = outer * inner
    slot_bits = slots.bit_length() - 1
    inner_bits = inner.bit_length() - 1
    piece_bits = pieces.bit_length() - 1

    x = lax.axis_index("gx")
    y = lax.axis_index("gy")
    q = lax.axis_index("gz")
    core = lax.rem(y, CORES)
    chip = y // CORES
    other = 1 - core
    own_rows = pl.ds(pl.multiple_of(core * LANES, LANES), LANES)
    other_rows = pl.ds(pl.multiple_of(other * LANES, LANES), LANES)

    def at(gx, gchip, gcore, gz):
        return (gx, gchip * CORES + gcore, gz)

    z_peers = [(k, lax.rem(x + k, outer)) for k in range(1, outer)]
    z_peers.sort(key=lambda p: -min(p[0], outer - p[0]))
    half = chips // 2
    column = lax.rem(chip, half)
    own_base = chip - column
    other_base = lax.rem(own_base + half, chips)
    across = other_base + column
    y_peer = at(x, across, core, q)
    x_peers = [(k, own_base + lax.rem(column + k, half)) for k in range(1, half)]
    gz_peers = [
        (dc * quarters + dq - 1, lax.rem(core + dc, CORES), lax.rem(q + dq, quarters))
        for dc in range(CORES)
        for dq in range(quarters)
        if dc or dq
    ]

    loads = [
        pltpu.make_async_copy(h_hbm, h2.at[core], local_sem.at[0]),
        pltpu.make_async_copy(cnt_hbm, cntv, local_sem.at[1]),
        pltpu.make_async_copy(wb_hbm, wbv, local_sem.at[2]),
        pltpu.make_async_copy(kg_hbm, kg2.at[own_rows], local_sem.at[3]),
        pltpu.make_async_copy(gain_hbm, gainv, local_sem.at[4]),
        pltpu.make_async_copy(ng_hbm, ngv, local_sem.at[5]),
    ]
    for copy in loads:
        copy.start()
    barrier = pltpu.get_barrier_semaphore()
    peers = [at(zx, chip, core, q) for _, zx in z_peers]
    peers += [y_peer] + [at(x, to, core, q) for _, to in x_peers]
    peers += [at(x, chip, gcore, gq) for _, gcore, gq in gz_peers]
    for peer in peers:
        pl.semaphore_signal(barrier, inc=1, device_id=peer, device_id_type=MESH)

    groups = lane_groups(rows)

    loads[0].wait()
    partial = jnp.zeros((LANES, LANES), F32)
    for g in groups:
        piece = h2[core, :, g].astype(F32)
        partial = partial + piece * piece
    row = jnp.sum(jnp.transpose(partial), axis=0, keepdims=True)
    sq[core, q] = jnp.broadcast_to(row, (8, LANES))

    loads[2].wait()
    own_blocks = jnp.concatenate(
        [wbv[0, 0].astype(F32), jnp.zeros((slots - most, LANES), F32)], axis=0
    )
    gathered[chip, x] = own_blocks.astype(BF16)
    loads[3].wait()

    pl.semaphore_wait(barrier, len(peers))

    sends = []

    def push(src, dst, send_sem, recv_sem, peer):
        copy = pltpu.make_async_remote_copy(
            src_ref=src, dst_ref=dst, send_sem=send_sem, recv_sem=recv_sem,
            device_id=peer, device_id_type=MESH,
        )
        copy.start()
        sends.append(copy)
        return copy

    sq_copies = [
        push(sq.at[core, q], sq.at[core, q], sq_s.at[m], sq_r.at[m], at(x, chip, gcore, gq))
        for m, gcore, gq in gz_peers
    ]
    c1_copies = [
        push(gathered.at[chip, x], gathered.at[chip, x], c1_s.at[k - 1], c1_r.at[k - 1], at(zx, chip, core, q))
        for k, zx in z_peers
    ]
    sibling = at(x, chip, other, q)
    sib_copies = [
        push(kg2.at[own_rows], kg2.at[own_rows], sib_s.at[0], sib_r.at[0], sibling),
        push(h2.at[core], h2.at[core], sib_s.at[1], sib_r.at[1], sibling),
    ]

    loads[1].wait()
    loads[4].wait()
    counts = cntv[...].astype(F32)
    owner_of = iota((padded_outer, owners), 1)
    of_group = (owner_of >> inner_bits) == iota((padded_outer, owners), 0)
    by_group = jnp.where(of_group, jnp.broadcast_to(counts, (padded_outer, owners)), 0.0).astype(BF16)

    def placed(shape, slot_dim, owner_dim):
        slot = iota(shape, slot_dim)
        holder = (slot >> slot_bits) * CORES + core
        within = iota(shape, owner_dim) & (inner - 1)
        before = jnp.where(within < holder, 1.0, 0.0).astype(BF16)
        mine = jnp.where(within == holder, 1.0, 0.0).astype(BF16)
        return before, mine

    before, mine = placed((per_group, owners), 0, 1)
    start_c = nt_dot(before, by_group).astype(jnp.int32)
    count_c = nt_dot(mine, by_group).astype(jnp.int32)
    within_c = iota((per_group, padded_outer), 0) & (slots - 1)
    block_c = start_c + within_c + group_blocks * iota((per_group, padded_outer), 1)
    block_c = jnp.where(within_c < count_c, block_c, -pieces)
    row_c = block_c >> piece_bits
    jcol[...] = block_c & (pieces - 1)
    start_r = nt_dot(by_group, before).astype(jnp.int32)
    count_r = nt_dot(by_group, mine).astype(jnp.int32)
    within_r = iota((padded_outer, per_group), 1) & (slots - 1)
    block_r = start_r + within_r + group_blocks * iota((padded_outer, per_group), 0)
    block_r = jnp.where(within_r < count_r, block_r, -pieces)
    row_r = block_r >> piece_bits

    def windows(z):
        first = group_blocks * z // pieces
        return (
            min(first // LANES * LANES, rows - lane_window),
            min(first // 8 * 8, rows - row_window),
        )

    for z in range(outer):
        lane0, row0 = windows(z)
        hit = row_c[:, z : z + 1] == lane0 + iota((per_group, lane_window), 1)
        onehot[z] = jnp.where(hit, 1.0, 0.0).astype(BF16)
        hit = row_r[z : z + 1, :] == row0 + iota((row_window, per_group), 0)
        onehot_t[z] = jnp.where(hit, 1.0, 0.0).astype(BF16)
    wfull[...] = jnp.zeros_like(wfull)

    for copy in sq_copies:
        copy.wait_recv()
    for copy in sib_copies:
        copy.wait_recv()
    for c in range(CORES):
        total = sq[c, 0, 0:1]
        for other_q in range(1, quarters):
            total = total + sq[c, other_q, 0:1]
        rs[c] = as_column(lax.rsqrt(total / model_width + EPS))
        for g in groups:
            scaled = h2[c, :, g].astype(F32) * rs[c] * gainv[:, g]
            nrm[c * LANES : (c + 1) * LANES, g] = scaled.astype(BF16)

    for copy in c1_copies:
        copy.wait_recv()
    own_slots = gathered.at[chip]
    c2_y = push(own_slots, own_slots, c2_s.at[0], c2_r.at[0], y_peer)
    c2_copies = [
        push(own_slots, own_slots, c2_s.at[k], c2_r.at[k], at(x, to, core, q)) for k, to in x_peers
    ]

    step = outer // BATCHES
    by_copies = []
    for batch in range(BATCHES):
        for z in range(batch * step, (batch + 1) * step):
            lane0, _ = windows(z)
            picked = nt_dot(onehot[z], nrm[:, lane0 : lane0 + lane_window]).astype(BF16)
            spread = jnp.dot(picked, kg2[...], preferred_element_type=F32)
            piece_of = jcol[:, z : z + 1]
            value = spread[:, :LANES]
            for j in range(1, pieces):
                value = jnp.where(piece_of == j, spread[:, j * LANES : (j + 1) * LANES], value)
            value = value.reshape(chips, slots, LANES)
            kept[:, z] = value
            y_send[:, z] = value.astype(BF16)
        span = pl.ds(batch * step, step)
        by_copies.append(push(
            y_send.at[pl.ds(other_base, half), span], y_recv.at[:, span], by_s.at[batch], by_r.at[batch], y_peer
        ))

    c2_y.wait_recv()
    c2_copies += [
        push(
            gathered.at[across], gathered.at[across], c2_s.at[half - 1 + k], c2_r.at[half - 1 + k],
            at(x, to, core, q),
        )
        for k, to in x_peers
    ]

    bx_copies = []
    for batch in range(BATCHES):
        by_copies[batch].wait_recv()
        for z in range(batch * step, (batch + 1) * step):
            kept[chip, z] = kept[chip, z] + y_recv[column, z].astype(F32)
            for k, to in x_peers:
                total = kept[to, z] + y_recv[to - own_base, z].astype(F32)
                x_send[k - 1, z] = total.astype(BF16)
        span = pl.ds(batch * step, step)
        bx_copies.append([
            push(
                x_send.at[k - 1, span], x_recv.at[k - 1, span], bx_s.at[k - 1, batch], bx_r.at[k - 1, batch],
                at(x, to, core, q),
            )
            for k, to in x_peers
        ])

    for copy in c2_copies:
        copy.wait_recv()
    for z in range(outer):
        _, row0 = windows(z)
        values = gathered[:, z].reshape(per_group, LANES)
        piece_of = jcol[:, z : z + 1]
        spread = jnp.concatenate(
            [jnp.where(piece_of == j, values, jnp.zeros_like(values)) for j in range(pieces)], axis=1
        )
        wfull[row0 : row0 + row_window, :] += jnp.dot(
            onehot_t[z], spread, preferred_element_type=F32
        )
    weight = wfull[...].astype(BF16)
    product[...] = nt_dot(kg2[...], weight)
    p_copy = push(product.at[other_rows], p_recv, sib_s.at[2], sib_r.at[2], sibling)

    def z_copy(k, zx, peer):
        return pltpu.make_async_remote_copy(
            src_ref=zsend.at[zx], dst_ref=zrecv.at[k - 1], send_sem=z_s.at[k - 1], recv_sem=z_r.at[k - 1],
            device_id=peer, device_id_type=MESH,
        )

    for batch in range(BATCHES):
        for copy in bx_copies[batch]:
            copy.wait_recv()
        for z in range(batch * step, (batch + 1) * step):
            total = kept[chip, z]
            for k, _ in x_peers:
                total = total + x_recv[k - 1, z].astype(F32)
            zsend[z] = total
        for z in range(batch * step, (batch + 1) * step):

            @pl.when(x != z)
            def _():
                z_copy(lax.rem(z - x + outer, outer), z, at(z, chip, core, q)).start()

    loads[5].wait()
    p_copy.wait_recv()
    partial = jnp.zeros((LANES, LANES), F32)
    for g in groups:
        dnorm = ngv[:, g].astype(F32) + (product[own_rows, g] + p_recv[:, g])
        gained = gainv[:, g] * dnorm
        p_recv[:, g] = gained
        partial = partial + gained * h2[core, :, g].astype(F32)
    row = jnp.sum(jnp.transpose(partial), axis=0, keepdims=True)
    pj[q] = jnp.broadcast_to(row, (8, LANES))
    pj_copies = [
        push(pj.at[q], pj.at[q], pj_s.at[dq - 1], pj_r.at[dq - 1], at(x, chip, core, lax.rem(q + dq, quarters)))
        for dq in range(1, quarters)
    ]
    for copy in pj_copies:
        copy.wait_recv()
    proj = pj[0, 0:1]
    for other_q in range(1, quarters):
        proj = proj + pj[other_q, 0:1]
    rstd = rs[core]
    coefficient = rstd * rstd * rstd * as_column(proj) / model_width
    for g in groups:
        grad = p_recv[:, g] * rstd - h2[core, :, g].astype(F32) * coefficient
        hg_ref[:, g] = grad.astype(BF16)

    for k, zx in z_peers:
        z_copy(k, zx, at(zx, chip, core, q)).wait_recv()
    total = zsend[x]
    for k in range(1, outer):
        total = total + zrecv[k - 1]
    wg_ref[0, 0] = total[:most]
    for k, zx in z_peers:
        z_copy(k, zx, at(zx, chip, core, q)).wait_send()
    for copy in sends:
        copy.wait_send()


def shards(hidden_in, norm_gain, normed_grad, key_grad, weight_blocks, block_count):
    outer, inner, quarters = lax.axis_size("gx"), lax.axis_size("gy"), lax.axis_size("gz")
    tokens, rows = hidden_in.shape
    width = key_grad.shape[1]
    most = weight_blocks.shape[2]
    blocks = rows * width // LANES
    pieces = width // LANES
    group_blocks = (blocks + outer - 1) // outer
    slots = round_up(most, 32)
    chips = inner // CORES
    half = chips // 2
    lines = max(half - 1, 1)
    per_group = chips * slots
    padded_outer = round_up(outer, 16)
    span = (group_blocks + pieces - 1) // pieces + 1
    cfg = dict(
        outer=outer, inner=inner, quarters=quarters, chips=chips, slots=slots, most=most,
        group_blocks=group_blocks, blocks=blocks, rows=rows, width=width, pieces=pieces,
        model_width=rows * quarters, padded_outer=padded_outer,
        lane_window=min(rows, round_up(span + LANES - 1, LANES)),
        row_window=min(rows, round_up(span + 7, 8)),
    )
    vmem = pltpu.VMEM
    dma = pltpu.SemaphoreType.DMA
    hg, wg = pl.pallas_call(
        functools.partial(kernel, cfg),
        out_shape=(
            pltpu.VMEM((tokens, rows), BF16),
            pltpu.VMEM(weight_blocks.shape, F32),
        ),
        in_specs=[pl.BlockSpec(memory_space=pltpu.HBM)] * 6,
        out_specs=(pl.BlockSpec(memory_space=pltpu.VMEM), pl.BlockSpec(memory_space=pltpu.VMEM)),
        scratch_shapes=[
            vmem((CORES, tokens, rows), BF16),
            vmem((1, rows), F32),
            vmem((tokens, rows), BF16),
            vmem((CORES * tokens, width), BF16),
            vmem(weight_blocks.shape, BF16),
            vmem(block_count.shape, jnp.int32),
            vmem((CORES, quarters, 8, LANES), F32),
            vmem((quarters, 8, LANES), F32),
            vmem((CORES, LANES, LANES), F32),
            vmem((CORES * tokens, rows), BF16),
            vmem((outer, per_group, cfg["lane_window"]), BF16),
            vmem((outer, cfg["row_window"], per_group), BF16),
            vmem((per_group, padded_outer), jnp.int32),
            vmem((chips, outer, slots, LANES), BF16),
            vmem((chips, outer, slots, LANES), F32),
            vmem((chips, outer, slots, LANES), BF16),
            vmem((half, outer, slots, LANES), BF16),
            vmem((lines, outer, slots, LANES), BF16),
            vmem((lines, outer, slots, LANES), BF16),
            vmem((outer, slots, LANES), F32),
            vmem((outer - 1, slots, LANES), F32),
            vmem((rows, width), F32),
            vmem((CORES * tokens, rows), F32),
            vmem((tokens, rows), F32),
            dma((6,)),
            dma((CORES * quarters - 1,)), dma((CORES * quarters - 1,)),
            dma((3,)), dma((3,)),
            dma((outer - 1,)), dma((outer - 1,)),
            dma((BATCHES,)), dma((BATCHES,)),
            dma((lines, BATCHES)), dma((lines, BATCHES)),
            dma((chips - 1,)), dma((chips - 1,)),
            dma((max(quarters - 1, 1),)), dma((max(quarters - 1, 1),)),
            dma((outer - 1,)), dma((outer - 1,)),
        ],
        compiler_params=pltpu.CompilerParams(
            collective_id=0, has_side_effects=True, vmem_limit_bytes=60_000_000
        ),
        name="key_projection_backward",
    )(hidden_in, norm_gain.reshape(1, rows), normed_grad, key_grad, weight_blocks, block_count)
    return hg, wg


def solution(mesh):
    placed = (
        P(("gx", "gy"), "gz"),
        P("gz"),
        P(("gx", "gy"), "gz"),
        P(("gx", "gy"), None),
        P(("gx", "gy"), "gz", None, None),
        P("gz", None),
    )
    return jax.shard_map(
        shards,
        mesh=mesh,
        in_specs=placed,
        out_specs=(P(("gx", "gy"), "gz"), P(("gx", "gy"), "gz", None, None)),
        check_vma=False,
    )
```

```python
import functools

import jax
import jax.numpy as jnp
from jax import lax
from jax.experimental import pallas as pl
from jax.experimental.pallas import tpu as pltpu
from jax.sharding import PartitionSpec as P

EPS = 1e-06
LANES = 128
CORES = 2
F32 = jnp.float32
BF16 = jnp.bfloat16
MESH = pl.DeviceIdType.MESH
BATCHES = (3, 3, 3, 2, 1)


def round_up(value, step):
    return (value + step - 1) // step * step


def iota(shape, dim):
    return lax.broadcasted_iota(jnp.int32, shape, dim)


def nt_dot(a, b):
    return lax.dot_general(a, b, (((1,), (1,)), ((), ())), preferred_element_type=F32)


def as_column(row):
    return jnp.transpose(jnp.broadcast_to(row, (LANES, LANES)))


def lane_groups(rows):
    return [slice(g * LANES, (g + 1) * LANES) for g in range(rows // LANES)]


def kernel(
    cfg,
    h_hbm, gain_hbm, ng_hbm, kg_hbm, wb_hbm, cnt_hbm,
    hg_ref, wg_ref,
    h2, gainv, ngv, kg2, wbv, cntv,
    sq, pj, rs, nrm, onehot, onehot_t, piece_of,
    gathered, kept, y_send, y_recv, x_send, x_recv, zsend, zrecv, wfull, product, p_recv,
    local_sem, send_sem, sib_sem, recv_sem, by_sem, bx_sem,
):
    outer, inner, quarters, chips = cfg["outer"], cfg["inner"], cfg["quarters"], cfg["chips"]
    slots, most, group_blocks, blocks = cfg["slots"], cfg["most"], cfg["group_blocks"], cfg["blocks"]
    rows, width, pieces, model_width = cfg["rows"], cfg["width"], cfg["pieces"], cfg["model_width"]
    lane_window, row_window, padded_outer = cfg["lane_window"], cfg["row_window"], cfg["padded_outer"]
    per_group = chips * slots
    owners = outer * inner
    slot_bits = slots.bit_length() - 1
    inner_bits = inner.bit_length() - 1
    piece_bits = pieces.bit_length() - 1

    x = lax.axis_index("gx")
    y = lax.axis_index("gy")
    q = lax.axis_index("gz")
    core = lax.rem(y, CORES)
    chip = y // CORES
    other = 1 - core
    own_rows = pl.ds(pl.multiple_of(core * LANES, LANES), LANES)
    other_rows = pl.ds(pl.multiple_of(other * LANES, LANES), LANES)

    def at(gx, gchip, gcore, gz):
        return (gx, gchip * CORES + gcore, gz)

    z_peers = [(k, lax.rem(x + k, outer)) for k in range(1, outer)]
    z_peers.sort(key=lambda p: -min(p[0], outer - p[0]))
    half = chips // 2
    column = lax.rem(chip, half)
    own_base = chip - column
    other_base = lax.rem(own_base + half, chips)
    across = other_base + column
    y_peer = at(x, across, core, q)
    x_peers = [(k, own_base + lax.rem(column + k, half)) for k in range(1, half)]
    SQ, C1, BY, BX, C2, PJ, ZZ = range(7)
    C2_Y, C2_OWN, C2_ACROSS = range(7, 10)
    gz_peers = [
        (dc * quarters + dq - 1, lax.rem(core + dc, CORES), lax.rem(q + dq, quarters))
        for dc in range(CORES)
        for dq in range(quarters)
        if dc or dq
    ]

    loads = [
        pltpu.make_async_copy(h_hbm, h2.at[core], local_sem.at[0]),
        pltpu.make_async_copy(cnt_hbm, cntv, local_sem.at[1]),
        pltpu.make_async_copy(wb_hbm, wbv, local_sem.at[2]),
        pltpu.make_async_copy(kg_hbm, kg2.at[own_rows], local_sem.at[3]),
        pltpu.make_async_copy(gain_hbm, gainv, local_sem.at[4]),
        pltpu.make_async_copy(ng_hbm, ngv, local_sem.at[5]),
    ]
    for copy in loads:
        copy.start()
    barrier = pltpu.get_barrier_semaphore()
    peers = [at(zx, chip, core, q) for _, zx in z_peers]
    peers += [y_peer] + [at(x, to, core, q) for _, to in x_peers]
    peers += [at(x, chip, gcore, gq) for _, gcore, gq in gz_peers]
    for peer in peers:
        pl.semaphore_signal(barrier, inc=1, device_id=peer, device_id_type=MESH)

    groups = lane_groups(rows)

    loads[0].wait()
    partial = jnp.zeros((LANES, LANES), F32)
    for g in groups:
        piece = h2[core, :, g].astype(F32)
        partial = partial + piece * piece
    row = jnp.sum(jnp.transpose(partial), axis=0, keepdims=True)
    sq[core * quarters + q] = jnp.broadcast_to(row, (8, LANES))

    loads[2].wait()
    own_blocks = jnp.concatenate(
        [wbv[0, 0].astype(F32), jnp.zeros((slots - most, LANES), F32)], axis=0
    )
    gathered[chip, x] = own_blocks.astype(BF16)
    loads[3].wait()

    pl.semaphore_wait(barrier, len(peers))

    def push(src, dst, sender, receiver, peer):
        copy = pltpu.make_async_remote_copy(
            src_ref=src, dst_ref=dst, send_sem=sender, recv_sem=receiver, device_id=peer, device_id_type=MESH
        )
        copy.start()

    def arrived(like, semaphore):
        pltpu.make_async_copy(like, like, semaphore).wait()

    own_sq = sq.at[core * quarters + q]
    for _, gcore, gq in gz_peers:
        push(own_sq, own_sq, send_sem.at[SQ], recv_sem.at[SQ], at(x, chip, gcore, gq))
    own_blocks = gathered.at[chip, x]
    for _, zx in z_peers:
        push(own_blocks, own_blocks, send_sem.at[C1], recv_sem.at[C1], at(zx, chip, core, q))
    sibling = at(x, chip, other, q)
    own_keys, own_hidden = kg2.at[own_rows], h2.at[core]
    push(own_keys, own_keys, sib_sem.at[0], sib_sem.at[1], sibling)
    push(own_hidden, own_hidden, sib_sem.at[2], sib_sem.at[3], sibling)

    loads[1].wait()
    loads[4].wait()
    counts = cntv[...].astype(F32)
    owner_of = iota((padded_outer, owners), 1)
    of_group = (owner_of >> inner_bits) == iota((padded_outer, owners), 0)
    by_group = jnp.where(of_group, jnp.broadcast_to(counts, (padded_outer, owners)), 0.0).astype(BF16)

    def placed(shape, slot_dim, owner_dim):
        slot = iota(shape, slot_dim)
        holder = (slot >> slot_bits) * CORES + core
        within = iota(shape, owner_dim) & (inner - 1)
        before = jnp.where(within < holder, 1.0, 0.0).astype(BF16)
        mine = jnp.where(within == holder, 1.0, 0.0).astype(BF16)
        return before, mine

    before, mine = placed((per_group, owners), 0, 1)
    start_c = nt_dot(before, by_group).astype(jnp.int32)
    count_c = nt_dot(mine, by_group).astype(jnp.int32)
    within_c = iota((per_group, padded_outer), 0) & (slots - 1)
    block_c = start_c + within_c + group_blocks * iota((per_group, padded_outer), 1)
    block_c = jnp.where(within_c < count_c, block_c, -pieces)
    row_c = block_c >> piece_bits
    piece_c = block_c & (pieces - 1)
    start_r = nt_dot(by_group, before).astype(jnp.int32)
    count_r = nt_dot(by_group, mine).astype(jnp.int32)
    within_r = iota((padded_outer, per_group), 1) & (slots - 1)
    block_r = start_r + within_r + group_blocks * iota((padded_outer, per_group), 0)
    block_r = jnp.where(within_r < count_r, block_r, -pieces)
    row_r = block_r >> piece_bits

    def first_lane(z):
        return group_blocks * z // pieces // LANES * LANES

    def first_row(z):
        return min(group_blocks * z // pieces // 8 * 8, rows - row_window)

    for z in range(outer):
        hit = row_c[:, z : z + 1] == first_lane(z) + iota((per_group, lane_window), 1)
        onehot[z] = jnp.where(hit, 1.0, 0.0).astype(BF16)
        hit = row_r[z : z + 1, :] == first_row(z) + iota((row_window, per_group), 0)
        onehot_t[z] = jnp.where(hit, 1.0, 0.0).astype(BF16)
        piece_of[z] = jnp.broadcast_to(piece_c[:, z : z + 1], (per_group, LANES))
    nrm[:, rows:] = jnp.zeros((CORES * LANES, LANES), BF16)
    wfull[...] = jnp.zeros_like(wfull)

    arrived(sq.at[pl.ds(0, len(gz_peers))], recv_sem.at[SQ])
    arrived(own_keys, sib_sem.at[1])
    arrived(own_hidden, sib_sem.at[3])
    for c in range(CORES):
        total = sq[c * quarters, 0:1]
        for other_q in range(1, quarters):
            total = total + sq[c * quarters + other_q, 0:1]
        rs[c] = as_column(lax.rsqrt(total / model_width + EPS))
        for g in groups:
            scaled = h2[c, :, g].astype(F32) * rs[c] * gainv[:, g]
            nrm[c * LANES : (c + 1) * LANES, g] = scaled.astype(BF16)

    offsets = sorted(range(outer), key=lambda k: -min(k, outer - k))
    ends = [sum(BATCHES[: b + 1]) for b in range(len(BATCHES))]
    spans = [(end - size, size) for end, size in zip(ends, BATCHES)]

    def slot_gradients(batch):
        start, size = spans[batch]
        for n in range(start, start + size):
            z = lax.rem(x + offsets[n], outer)
            lanes = pl.ds(pl.multiple_of(first_lane(z), LANES), lane_window)
            picked = nt_dot(onehot[z], nrm[:, lanes]).astype(BF16)
            spread = jnp.dot(picked, kg2[...], preferred_element_type=F32)
            value = spread[:, :LANES]
            for j in range(1, pieces):
                value = jnp.where(piece_of[z] == j, spread[:, j * LANES : (j + 1) * LANES], value)
            value = value.reshape(chips, slots, LANES)
            kept[:, n] = value
            y_send[:, n] = value.astype(BF16)
        span = pl.ds(start, size)
        push(
            y_send.at[pl.ds(other_base, half), span], y_recv.at[:, span], send_sem.at[BY], by_sem.at[batch], y_peer
        )

    def along_x(batch):
        start, size = spans[batch]
        span = pl.ds(start, size)
        arrived(y_recv.at[:, span], by_sem.at[batch])
        for n in range(start, start + size):
            kept[chip, n] = kept[chip, n] + y_recv[column, n].astype(F32)
            for k, to in x_peers:
                total = kept[to, n] + y_recv[to - own_base, n].astype(F32)
                x_send[k - 1, n] = total.astype(BF16)
        for k, to in x_peers:
            push(
                x_send.at[k - 1, span], x_recv.at[k - 1, span], send_sem.at[BX], bx_sem.at[batch],
                at(x, to, core, q),
            )

    def along_z(batch):
        start, size = spans[batch]
        span = pl.ds(start, size)
        if x_peers:
            arrived(x_recv.at[:, span], bx_sem.at[batch])
        for n in range(start, start + size):
            total = kept[chip, n]
            for k, _ in x_peers:
                total = total + x_recv[k - 1, n].astype(F32)
            zsend[n] = total
            if offsets[n]:
                push(
                    zsend.at[n], zrecv.at[n], send_sem.at[ZZ], recv_sem.at[ZZ],
                    at(lax.rem(x + offsets[n], outer), chip, core, q),
                )

    if z_peers:
        arrived(gathered.at[chip, pl.ds(0, outer - 1)], recv_sem.at[C1])
    def share(source, receiver, peers):
        held = gathered.at[source]
        for to in peers:
            push(held, held, send_sem.at[C2], recv_sem.at[receiver], at(x, to, core, q))

    along = [to for _, to in x_peers]
    share(chip, C2_Y, [across])
    share(chip, C2_OWN, along)
    batches = range(len(BATCHES))
    for batch in batches:
        slot_gradients(batch)
    arrived(gathered.at[across], recv_sem.at[C2_Y])
    share(across, C2_ACROSS, along)
    for batch in batches:
        along_x(batch)
    for batch in batches[:1]:
        along_z(batch)
    if along:
        arrived(gathered.at[pl.ds(0, len(along))], recv_sem.at[C2_OWN])
        arrived(gathered.at[pl.ds(0, len(along))], recv_sem.at[C2_ACROSS])
    for z in range(outer):
        row0 = first_row(z)
        values = gathered[:, z].reshape(per_group, LANES)
        spread = jnp.concatenate(
            [jnp.where(piece_of[z] == j, values, jnp.zeros_like(values)) for j in range(pieces)], axis=1
        )
        wfull[row0 : row0 + row_window, :] += jnp.dot(
            onehot_t[z], spread, preferred_element_type=F32
        )
    weight = wfull[...].astype(BF16)
    product[...] = nt_dot(kg2[...], weight)
    push(product.at[other_rows], p_recv, sib_sem.at[4], sib_sem.at[5], sibling)
    for batch in batches[1:3]:
        along_z(batch)

    loads[5].wait()
    arrived(p_recv, sib_sem.at[5])
    partial = jnp.zeros((LANES, LANES), F32)
    for g in groups:
        dnorm = ngv[:, g].astype(F32) + (product[own_rows, g] + p_recv[:, g])
        gained = gainv[:, g] * dnorm
        p_recv[:, g] = gained
        partial = partial + gained * h2[core, :, g].astype(F32)
    row = jnp.sum(jnp.transpose(partial), axis=0, keepdims=True)
    pj[q] = jnp.broadcast_to(row, (8, LANES))
    own_pj = pj.at[q]
    for dq in range(1, quarters):
        push(own_pj, own_pj, send_sem.at[PJ], recv_sem.at[PJ], at(x, chip, core, lax.rem(q + dq, quarters)))
    for batch in batches[3:]:
        along_z(batch)
    if quarters > 1:
        arrived(pj.at[pl.ds(0, quarters - 1)], recv_sem.at[PJ])
    proj = pj[0, 0:1]
    for other_q in range(1, quarters):
        proj = proj + pj[other_q, 0:1]
    rstd = rs[core]
    coefficient = rstd * rstd * rstd * as_column(proj) / model_width
    for g in groups:
        grad = p_recv[:, g] * rstd - h2[core, :, g].astype(F32) * coefficient
        hg_ref[:, g] = grad.astype(BF16)

    if z_peers:
        arrived(zrecv, recv_sem.at[ZZ])
    total = zsend[outer - 1]
    for n in range(outer - 1):
        total = total + zrecv[n]
    wg_ref[0, 0] = total[:most]
    arrived(sq.at[pl.ds(0, len(gz_peers))], send_sem.at[SQ])
    arrived(own_keys, sib_sem.at[0])
    arrived(own_hidden, sib_sem.at[2])
    arrived(p_recv, sib_sem.at[4])
    arrived(y_recv, send_sem.at[BY])
    arrived(gathered.at[pl.ds(0, chips - 1)], send_sem.at[C2])
    if x_peers:
        arrived(x_recv, send_sem.at[BX])
    if z_peers:
        arrived(gathered.at[0, pl.ds(0, outer - 1)], send_sem.at[C1])
        arrived(zrecv, send_sem.at[ZZ])
    if quarters > 1:
        arrived(pj.at[pl.ds(0, quarters - 1)], send_sem.at[PJ])


def finish(most, hg_ref, wg_ref, hg_out, wg_out, lines, sem):
    wide = pltpu.make_async_copy(hg_ref, hg_out, sem.at[0])
    wide.start()
    for row in range(most):
        lines[row] = wg_ref[0, 0, row : row + 1, :]
    narrow = pltpu.make_async_copy(lines, wg_out, sem.at[1])
    narrow.start()
    wide.wait()
    narrow.wait()


def shards(hidden_in, norm_gain, normed_grad, key_grad, weight_blocks, block_count):
    outer, inner, quarters = lax.axis_size("gx"), lax.axis_size("gy"), lax.axis_size("gz")
    tokens, rows = hidden_in.shape
    width = key_grad.shape[1]
    most = weight_blocks.shape[2]
    blocks = rows * width // LANES
    pieces = width // LANES
    group_blocks = (blocks + outer - 1) // outer
    slots = round_up(most, 32)
    chips = inner // CORES
    half = chips // 2
    lines = max(half - 1, 1)
    per_group = chips * slots
    padded_outer = round_up(outer, 16)
    span = (group_blocks + pieces - 1) // pieces + 1
    cfg = dict(
        outer=outer, inner=inner, quarters=quarters, chips=chips, slots=slots, most=most,
        group_blocks=group_blocks, blocks=blocks, rows=rows, width=width, pieces=pieces,
        model_width=rows * quarters, padded_outer=padded_outer,
        lane_window=min(rows, round_up(span + LANES - 1, LANES)),
        row_window=min(rows, round_up(span + 7, 8)),
    )
    vmem = pltpu.VMEM
    dma = pltpu.SemaphoreType.DMA
    hg, wg = pl.pallas_call(
        functools.partial(kernel, cfg),
        out_shape=(
            pltpu.VMEM((tokens, rows), BF16),
            pltpu.VMEM(weight_blocks.shape, F32),
        ),
        in_specs=[pl.BlockSpec(memory_space=pltpu.HBM)] * 6,
        out_specs=(pl.BlockSpec(memory_space=pltpu.VMEM), pl.BlockSpec(memory_space=pltpu.VMEM)),
        scratch_shapes=[
            vmem((CORES, tokens, rows), BF16),
            vmem((1, rows), F32),
            vmem((tokens, rows), BF16),
            vmem((CORES * tokens, width), BF16),
            vmem(weight_blocks.shape, BF16),
            vmem(block_count.shape, jnp.int32),
            vmem((CORES * quarters, 8, LANES), F32),
            vmem((quarters, 8, LANES), F32),
            vmem((CORES, LANES, LANES), F32),
            vmem((CORES * tokens, rows + LANES), BF16),
            vmem((outer, per_group, cfg["lane_window"]), BF16),
            vmem((outer, cfg["row_window"], per_group), BF16),
            vmem((outer, per_group, LANES), jnp.int32),
            vmem((chips, outer, slots, LANES), BF16),
            vmem((chips, outer, slots, LANES), F32),
            vmem((chips, outer, slots, LANES), BF16),
            vmem((half, outer, slots, LANES), BF16),
            vmem((lines, outer, slots, LANES), BF16),
            vmem((lines, outer, slots, LANES), BF16),
            vmem((outer, slots, LANES), F32),
            vmem((max(outer - 1, 1), slots, LANES), F32),
            vmem((rows, width), F32),
            vmem((CORES * tokens, rows), F32),
            vmem((tokens, rows), F32),
            dma((6,)), dma((7,)), dma((6,)), dma((10,)), dma((len(BATCHES),)), dma((len(BATCHES),)),
        ],
        compiler_params=pltpu.CompilerParams(
            collective_id=0, has_side_effects=True, vmem_limit_bytes=60_000_000
        ),
        name="key_projection_backward",
    )(hidden_in, norm_gain.reshape(1, rows), normed_grad, key_grad, weight_blocks, block_count)
    hg, wg = pl.pallas_call(
        functools.partial(finish, most),
        out_shape=(
            jax.ShapeDtypeStruct((tokens, rows), BF16),
            jax.ShapeDtypeStruct((most, 1, LANES), F32),
        ),
        in_specs=[pl.BlockSpec(memory_space=pltpu.VMEM)] * 2,
        out_specs=[pl.BlockSpec(memory_space=pltpu.HBM)] * 2,
        scratch_shapes=[vmem((most, 1, LANES), F32), dma((2,))],
        compiler_params=pltpu.CompilerParams(vmem_limit_bytes=2 * 1024 * 1024),
        name="write_results",
    )(hg, wg)
    return hg, wg.reshape(weight_blocks.shape)


def solution(mesh):
    placed = (
        P(("gx", "gy"), "gz"),
        P("gz"),
        P(("gx", "gy"), "gz"),
        P(("gx", "gy"), None),
        P(("gx", "gy"), "gz", None, None),
        P("gz", None),
    )
    return jax.shard_map(
        shards,
        mesh=mesh,
        in_specs=placed,
        out_specs=(P(("gx", "gy"), "gz"), P(("gx", "gy"), "gz", None, None)),
        check_vma=False,
    )
```

```python
import functools

import jax
import jax.numpy as jnp
from jax import lax
from jax.experimental import pallas as pl
from jax.experimental.pallas import tpu as pltpu
from jax.sharding import PartitionSpec as P

EPS = 1e-06
LANES = 128
CORES = 2
F32 = jnp.float32
BF16 = jnp.bfloat16
MESH = pl.DeviceIdType.MESH
BATCHES = (3, 3, 3, 2, 1)


def round_up(value, step):
    return (value + step - 1) // step * step


def iota(shape, dim):
    return lax.broadcasted_iota(jnp.int32, shape, dim)


def nt_dot(a, b):
    return lax.dot_general(a, b, (((1,), (1,)), ((), ())), preferred_element_type=F32)


def as_column(row):
    return jnp.transpose(jnp.broadcast_to(row, (LANES, LANES)))


def lane_groups(rows):
    return [slice(g * LANES, (g + 1) * LANES) for g in range(rows // LANES)]


def kernel(
    cfg,
    h_hbm, gain_hbm, ng_hbm, kg_hbm, wb_hbm, cnt_hbm,
    hg_ref, wg_ref,
    h2, gainv, ngv, kg2, wbv, cntv,
    sq, pj, rs, nrm, onehot, onehot_t, piece_of,
    proj_early, pj_other, gathered, kept, y_send, y_recv, x_send, x_recv, zsend, zrecv, wfull, product, p_recv,
    local_sem, send_sem, sib_sem, recv_sem, by_sem, bx_sem,
):
    outer, inner, quarters, chips = cfg["outer"], cfg["inner"], cfg["quarters"], cfg["chips"]
    slots, most, group_blocks, blocks = cfg["slots"], cfg["most"], cfg["group_blocks"], cfg["blocks"]
    rows, width, pieces, model_width = cfg["rows"], cfg["width"], cfg["pieces"], cfg["model_width"]
    lane_window, row_window, padded_outer = cfg["lane_window"], cfg["row_window"], cfg["padded_outer"]
    per_group = chips * slots
    owners = outer * inner
    slot_bits = slots.bit_length() - 1
    inner_bits = inner.bit_length() - 1
    piece_bits = pieces.bit_length() - 1

    x = lax.axis_index("gx")
    y = lax.axis_index("gy")
    q = lax.axis_index("gz")
    core = lax.rem(y, CORES)
    chip = y // CORES
    other = 1 - core
    own_rows = pl.ds(pl.multiple_of(core * LANES, LANES), LANES)
    other_rows = pl.ds(pl.multiple_of(other * LANES, LANES), LANES)

    def at(gx, gchip, gcore, gz):
        return (gx, gchip * CORES + gcore, gz)

    z_peers = [(k, lax.rem(x + k, outer)) for k in range(1, outer)]
    z_peers.sort(key=lambda p: min(p[0], outer - p[0]))
    half = chips // 2
    column = lax.rem(chip, half)
    own_base = chip - column
    other_base = lax.rem(own_base + half, chips)
    across = other_base + column
    y_peer = at(x, across, core, q)
    x_peers = [(k, own_base + lax.rem(column + k, half)) for k in range(1, half)]
    SQ, C1, BY, BX, C2, PJ, ZZ = range(7)
    C1_FAR, C2_Y, C2_Y_FAR, C2_OWN, C2_ACROSS = range(7, 12)
    gz_peers = [
        (dc * quarters + dq - 1, lax.rem(core + dc, CORES), lax.rem(q + dq, quarters))
        for dc in range(CORES)
        for dq in range(quarters)
        if dc or dq
    ]

    offsets = sorted(range(outer), key=lambda k: -min(k, outer - k))
    place = [offsets.index(k) for k in range(outer)]
    far = sum(min(k, outer - k) > 3 for k in offsets)
    far_planes, near_planes = pl.ds(0, far), pl.ds(far, outer - far)

    loads = [
        pltpu.make_async_copy(h_hbm, h2.at[core], local_sem.at[0]),
        pltpu.make_async_copy(cnt_hbm, cntv, local_sem.at[1]),
        pltpu.make_async_copy(wb_hbm, wbv, local_sem.at[2]),
        pltpu.make_async_copy(kg_hbm, kg2.at[own_rows], local_sem.at[3]),
        pltpu.make_async_copy(gain_hbm, gainv, local_sem.at[4]),
        pltpu.make_async_copy(ng_hbm, ngv, local_sem.at[5]),
    ]
    for copy in loads:
        copy.start()
    barrier = pltpu.get_barrier_semaphore()
    peers = [at(zx, chip, core, q) for _, zx in z_peers]
    peers += [y_peer] + [at(x, to, core, q) for _, to in x_peers]
    peers += [at(x, chip, gcore, gq) for _, gcore, gq in gz_peers]
    for peer in peers:
        pl.semaphore_signal(barrier, inc=1, device_id=peer, device_id_type=MESH)

    groups = lane_groups(rows)

    loads[0].wait()
    partial = jnp.zeros((LANES, LANES), F32)
    for g in groups:
        piece = h2[core, :, g].astype(F32)
        partial = partial + piece * piece
    row = jnp.sum(jnp.transpose(partial), axis=0, keepdims=True)
    sq[core * quarters + q] = jnp.broadcast_to(row, (8, LANES))

    loads[2].wait()
    own_blocks = jnp.concatenate(
        [wbv[0, 0].astype(F32), jnp.zeros((slots - most, LANES), F32)], axis=0
    )
    gathered[chip, outer - 1] = own_blocks.astype(BF16)
    loads[3].wait()

    pl.semaphore_wait(barrier, len(peers))

    def push(src, dst, sender, receiver, peer):
        copy = pltpu.make_async_remote_copy(
            src_ref=src, dst_ref=dst, send_sem=sender, recv_sem=receiver, device_id=peer, device_id_type=MESH
        )
        copy.start()

    def arrived(like, semaphore):
        pltpu.make_async_copy(like, like, semaphore).wait()

    own_sq = sq.at[core * quarters + q]
    for _, gcore, gq in gz_peers:
        push(own_sq, own_sq, send_sem.at[SQ], recv_sem.at[SQ], at(x, chip, gcore, gq))
    own_blocks = gathered.at[chip, outer - 1]
    for k, zx in z_peers:
        spot = place[outer - k]
        push(
            own_blocks, gathered.at[chip, spot], send_sem.at[C1], recv_sem.at[C1_FAR if spot < far else C1],
            at(zx, chip, core, q),
        )
    sibling = at(x, chip, other, q)
    own_keys, own_hidden = kg2.at[own_rows], h2.at[core]
    push(own_keys, own_keys, sib_sem.at[0], sib_sem.at[1], sibling)
    push(own_hidden, own_hidden, sib_sem.at[2], sib_sem.at[3], sibling)

    loads[1].wait()
    loads[4].wait()
    counts = cntv[...].astype(F32)
    owner_of = iota((padded_outer, owners), 1)
    of_group = (owner_of >> inner_bits) == iota((padded_outer, owners), 0)
    by_group = jnp.where(of_group, jnp.broadcast_to(counts, (padded_outer, owners)), 0.0).astype(BF16)

    def placed(shape, slot_dim, owner_dim):
        slot = iota(shape, slot_dim)
        holder = (slot >> slot_bits) * CORES + core
        within = iota(shape, owner_dim) & (inner - 1)
        before = jnp.where(within < holder, 1.0, 0.0).astype(BF16)
        mine = jnp.where(within == holder, 1.0, 0.0).astype(BF16)
        return before, mine

    before, mine = placed((per_group, owners), 0, 1)
    start_c = nt_dot(before, by_group).astype(jnp.int32)
    count_c = nt_dot(mine, by_group).astype(jnp.int32)
    within_c = iota((per_group, padded_outer), 0) & (slots - 1)
    block_c = start_c + within_c + group_blocks * iota((per_group, padded_outer), 1)
    block_c = jnp.where(within_c < count_c, block_c, -pieces)
    row_c = block_c >> piece_bits
    piece_c = block_c & (pieces - 1)
    start_r = nt_dot(by_group, before).astype(jnp.int32)
    count_r = nt_dot(by_group, mine).astype(jnp.int32)
    within_r = iota((padded_outer, per_group), 1) & (slots - 1)
    block_r = start_r + within_r + group_blocks * iota((padded_outer, per_group), 0)
    block_r = jnp.where(within_r < count_r, block_r, -pieces)
    row_r = block_r >> piece_bits

    def first_lane(z):
        return group_blocks * z // pieces // LANES * LANES

    def first_row(z):
        return group_blocks * z // pieces // 8 * 8

    for z in range(outer):
        hit = row_c[:, z : z + 1] == first_lane(z) + iota((per_group, lane_window), 1)
        onehot[z] = jnp.where(hit, 1.0, 0.0).astype(BF16)
        hit = row_r[z : z + 1, :] == first_row(z) + iota((row_window, per_group), 0)
        onehot_t[z] = jnp.where(hit, 1.0, 0.0).astype(BF16)
        piece_of[z] = jnp.broadcast_to(piece_c[:, z : z + 1], (per_group, LANES))
    nrm[:, rows:] = jnp.zeros((CORES * LANES, LANES), BF16)
    wfull[...] = jnp.zeros_like(wfull)

    loads[5].wait()
    partial = jnp.zeros((LANES, LANES), F32)
    for g in groups:
        partial = partial + gainv[:, g] * ngv[:, g].astype(F32) * h2[core, :, g].astype(F32)
    proj_early[...] = partial

    def share(source, receiver, peers, planes):
        held = gathered.at[source, planes]
        for to in peers:
            push(held, held, send_sem.at[C2], recv_sem.at[receiver], at(x, to, core, q))

    along = [to for _, to in x_peers]

    arrived(sq.at[pl.ds(0, len(gz_peers))], recv_sem.at[SQ])
    arrived(own_keys, sib_sem.at[1])
    arrived(own_hidden, sib_sem.at[3])
    for c in range(CORES):
        total = sq[c * quarters, 0:1]
        for other_q in range(1, quarters):
            total = total + sq[c * quarters + other_q, 0:1]
        rs[c] = as_column(lax.rsqrt(total / model_width + EPS))
        for g in groups:
            scaled = h2[c, :, g].astype(F32) * rs[c] * gainv[:, g]
            nrm[c * LANES : (c + 1) * LANES, g] = scaled.astype(BF16)

    ends = [sum(BATCHES[: b + 1]) for b in range(len(BATCHES))]
    spans = [(end - size, size) for end, size in zip(ends, BATCHES)]

    def slot_gradients(batch):
        start, size = spans[batch]
        for n in range(start, start + size):
            z = lax.rem(x + offsets[n], outer)
            lanes = pl.ds(pl.multiple_of(first_lane(z), LANES), lane_window)
            picked = nt_dot(onehot[z], nrm[:, lanes]).astype(BF16)
            spread = jnp.dot(picked, kg2[...], preferred_element_type=F32)
            value = spread[:, :LANES]
            for j in range(1, pieces):
                value = jnp.where(piece_of[z] == j, spread[:, j * LANES : (j + 1) * LANES], value)
            value = value.reshape(chips, slots, LANES)
            kept[:, n] = value
            y_send[:, n] = value.astype(BF16)
        span = pl.ds(start, size)
        push(
            y_send.at[pl.ds(other_base, half), span], y_recv.at[:, span], send_sem.at[BY], by_sem.at[batch], y_peer
        )

    def along_x(batch):
        start, size = spans[batch]
        span = pl.ds(start, size)
        arrived(y_recv.at[:, span], by_sem.at[batch])
        for n in range(start, start + size):
            kept[chip, n] = kept[chip, n] + y_recv[column, n].astype(F32)
            for k, to in x_peers:
                total = kept[to, n] + y_recv[to - own_base, n].astype(F32)
                x_send[k - 1, n] = total.astype(BF16)
        for k, to in x_peers:
            push(
                x_send.at[k - 1, span], x_recv.at[k - 1, span], send_sem.at[BX], bx_sem.at[batch],
                at(x, to, core, q),
            )

    def along_z(batch):
        start, size = spans[batch]
        span = pl.ds(start, size)
        if x_peers:
            arrived(x_recv.at[:, span], bx_sem.at[batch])
        for n in range(start, start + size):
            total = kept[chip, n]
            for k, _ in x_peers:
                total = total + x_recv[k - 1, n].astype(F32)
            zsend[n] = total
            if offsets[n]:
                push(
                    zsend.at[n], zrecv.at[n], send_sem.at[ZZ], recv_sem.at[ZZ],
                    at(lax.rem(x + offsets[n], outer), chip, core, q),
                )

    if outer - far > 1:
        arrived(gathered.at[chip, pl.ds(far, outer - far - 1)], recv_sem.at[C1])
    share(chip, C2_Y, [across], near_planes)
    share(chip, C2_OWN, along, near_planes)
    batches = range(len(BATCHES))
    for batch in batches[:1]:
        slot_gradients(batch)
    if far:
        arrived(gathered.at[chip, far_planes], recv_sem.at[C1_FAR])
        share(chip, C2_Y_FAR, [across], far_planes)
        share(chip, C2_OWN, along, far_planes)
    for batch in batches[1:2]:
        slot_gradients(batch)
    arrived(gathered.at[across, near_planes], recv_sem.at[C2_Y])
    share(across, C2_ACROSS, along, near_planes)
    for batch in batches[2:]:
        slot_gradients(batch)
    along_x(0)
    if far:
        arrived(gathered.at[across, far_planes], recv_sem.at[C2_Y_FAR])
        share(across, C2_ACROSS, along, far_planes)
    for batch in batches[1:]:
        along_x(batch)
        if batch == 3:
            along_z(0)
    if along:
        arrived(gathered.at[pl.ds(0, len(along))], recv_sem.at[C2_OWN])
        arrived(gathered.at[pl.ds(0, len(along))], recv_sem.at[C2_ACROSS])
    for n in range(outer):
        z = lax.rem(x + offsets[n], outer)
        spread_rows = pl.ds(pl.multiple_of(first_row(z), 8), row_window)
        values = gathered[:, n].reshape(per_group, LANES)
        spread = jnp.concatenate(
            [jnp.where(piece_of[z] == j, values, jnp.zeros_like(values)) for j in range(pieces)], axis=1
        )
        wfull[spread_rows, :] += jnp.dot(
            onehot_t[z], spread, preferred_element_type=F32
        )
    weight = wfull[:rows].astype(BF16)
    product[...] = nt_dot(kg2[...], weight)
    push(product.at[other_rows], p_recv, sib_sem.at[4], sib_sem.at[5], sibling)
    partial = proj_early[...]
    part_other = jnp.zeros((LANES, LANES), F32)
    for g in groups:
        partial = partial + gainv[:, g] * h2[core, :, g].astype(F32) * product[own_rows, g]
        part_other = part_other + gainv[:, g] * h2[other, :, g].astype(F32) * product[other_rows, g]
    own_pj = pj.at[core * quarters + q]
    pj[core * quarters + q] = jnp.broadcast_to(jnp.sum(jnp.transpose(partial), axis=0, keepdims=True), (8, LANES))
    pj_other[...] = jnp.broadcast_to(jnp.sum(jnp.transpose(part_other), axis=0, keepdims=True), (8, LANES))
    for m, gcore, gq in gz_peers:
        push(
            own_pj if m < quarters - 1 else pj_other, own_pj, send_sem.at[PJ], recv_sem.at[PJ],
            at(x, chip, gcore, gq),
        )
    for batch in batches[0 if len(batches) < 4 else 1 : 3]:
        along_z(batch)

    arrived(p_recv, sib_sem.at[5])
    for g in groups:
        dnorm = ngv[:, g].astype(F32) + (product[own_rows, g] + p_recv[:, g])
        p_recv[:, g] = gainv[:, g] * dnorm
    for batch in batches[3:]:
        along_z(batch)
    arrived(pj.at[pl.ds(0, len(gz_peers))], recv_sem.at[PJ])
    proj = pj[0, 0:1]
    for m in range(1, CORES * quarters):
        proj = proj + pj[m, 0:1]
    rstd = rs[core]
    coefficient = rstd * rstd * rstd * as_column(proj) / model_width
    for g in groups:
        grad = p_recv[:, g] * rstd - h2[core, :, g].astype(F32) * coefficient
        hg_ref[:, g] = grad.astype(BF16)

    if z_peers:
        arrived(zrecv, recv_sem.at[ZZ])
    total = zsend[outer - 1]
    for n in range(outer - 1):
        total = total + zrecv[n]
    wg_ref[0, 0] = total[:most]
    arrived(sq.at[pl.ds(0, len(gz_peers))], send_sem.at[SQ])
    arrived(own_keys, sib_sem.at[0])
    arrived(own_hidden, sib_sem.at[2])
    arrived(p_recv, sib_sem.at[4])
    arrived(y_recv, send_sem.at[BY])
    arrived(gathered.at[pl.ds(0, chips - 1)], send_sem.at[C2])
    if x_peers:
        arrived(x_recv, send_sem.at[BX])
    if z_peers:
        arrived(gathered.at[0, pl.ds(0, outer - 1)], send_sem.at[C1])
        arrived(zrecv, send_sem.at[ZZ])
    arrived(pj.at[pl.ds(0, len(gz_peers))], send_sem.at[PJ])


def finish(most, hg_ref, wg_ref, hg_out, wg_out, lines, sem):
    wide = pltpu.make_async_copy(hg_ref, hg_out, sem.at[0])
    wide.start()
    for row in range(most):
        lines[row] = wg_ref[0, 0, row : row + 1, :]
    narrow = pltpu.make_async_copy(lines, wg_out, sem.at[1])
    narrow.start()
    wide.wait()
    narrow.wait()


def shards(hidden_in, norm_gain, normed_grad, key_grad, weight_blocks, block_count):
    outer, inner, quarters = lax.axis_size("gx"), lax.axis_size("gy"), lax.axis_size("gz")
    tokens, rows = hidden_in.shape
    width = key_grad.shape[1]
    most = weight_blocks.shape[2]
    blocks = rows * width // LANES
    pieces = width // LANES
    group_blocks = (blocks + outer - 1) // outer
    slots = round_up(most, 32)
    chips = inner // CORES
    half = chips // 2
    lines = max(half - 1, 1)
    per_group = chips * slots
    padded_outer = round_up(outer, 16)
    span = (group_blocks + pieces - 1) // pieces + 1
    cfg = dict(
        outer=outer, inner=inner, quarters=quarters, chips=chips, slots=slots, most=most,
        group_blocks=group_blocks, blocks=blocks, rows=rows, width=width, pieces=pieces,
        model_width=rows * quarters, padded_outer=padded_outer,
        lane_window=min(rows, round_up(span + LANES - 1, LANES)),
        row_window=min(rows, round_up(span + 7, 8)),
    )
    vmem = pltpu.VMEM
    dma = pltpu.SemaphoreType.DMA
    hg, wg = pl.pallas_call(
        functools.partial(kernel, cfg),
        out_shape=(
            pltpu.VMEM((tokens, rows), BF16),
            pltpu.VMEM(weight_blocks.shape, F32),
        ),
        in_specs=[pl.BlockSpec(memory_space=pltpu.HBM)] * 6,
        out_specs=(pl.BlockSpec(memory_space=pltpu.VMEM), pl.BlockSpec(memory_space=pltpu.VMEM)),
        scratch_shapes=[
            vmem((CORES, tokens, rows), BF16),
            vmem((1, rows), F32),
            vmem((tokens, rows), BF16),
            vmem((CORES * tokens, width), BF16),
            vmem(weight_blocks.shape, BF16),
            vmem(block_count.shape, jnp.int32),
            vmem((CORES * quarters, 8, LANES), F32),
            vmem((CORES * quarters, 8, LANES), F32),
            vmem((CORES, LANES, LANES), F32),
            vmem((CORES * tokens, rows + LANES), BF16),
            vmem((outer, per_group, cfg["lane_window"]), BF16),
            vmem((outer, cfg["row_window"], per_group), BF16),
            vmem((outer, per_group, LANES), jnp.int32),
            vmem((LANES, LANES), F32),
            vmem((8, LANES), F32),
            vmem((chips, outer, slots, LANES), BF16),
            vmem((chips, outer, slots, LANES), F32),
            vmem((chips, outer, slots, LANES), BF16),
            vmem((half, outer, slots, LANES), BF16),
            vmem((lines, outer, slots, LANES), BF16),
            vmem((lines, outer, slots, LANES), BF16),
            vmem((outer, slots, LANES), F32),
            vmem((max(outer - 1, 1), slots, LANES), F32),
            vmem((rows + cfg["row_window"], width), F32),
            vmem((CORES * tokens, rows), F32),
            vmem((tokens, rows), F32),
            dma((6,)), dma((7,)), dma((6,)), dma((12,)), dma((len(BATCHES),)), dma((len(BATCHES),)),
        ],
        compiler_params=pltpu.CompilerParams(
            collective_id=0, has_side_effects=True, vmem_limit_bytes=60_000_000
        ),
        name="key_projection_backward",
    )(hidden_in, norm_gain.reshape(1, rows), normed_grad, key_grad, weight_blocks, block_count)
    hg, wg = pl.pallas_call(
        functools.partial(finish, most),
        out_shape=(
            jax.ShapeDtypeStruct((tokens, rows), BF16),
            jax.ShapeDtypeStruct((most, 1, LANES), F32),
        ),
        in_specs=[pl.BlockSpec(memory_space=pltpu.VMEM)] * 2,
        out_specs=[pl.BlockSpec(memory_space=pltpu.HBM)] * 2,
        scratch_shapes=[vmem((most, 1, LANES), F32), dma((2,))],
        compiler_params=pltpu.CompilerParams(vmem_limit_bytes=2 * 1024 * 1024),
        name="write_results",
    )(hg, wg)
    return hg, wg.reshape(weight_blocks.shape)


def solution(mesh):
    placed = (
        P(("gx", "gy"), "gz"),
        P("gz"),
        P(("gx", "gy"), "gz"),
        P(("gx", "gy"), None),
        P(("gx", "gy"), "gz", None, None),
        P("gz", None),
    )
    return jax.shard_map(
        shards,
        mesh=mesh,
        in_specs=placed,
        out_specs=(P(("gx", "gy"), "gz"), P(("gx", "gy"), "gz", None, None)),
        check_vma=False,
    )
```

```python
import functools

import jax
import jax.numpy as jnp
from jax import lax
from jax.experimental import pallas as pl
from jax.experimental.pallas import tpu as pltpu
from jax.sharding import PartitionSpec as P

EPS = 1e-06
LANES = 128
CORES = 2
F32 = jnp.float32
BF16 = jnp.bfloat16
MESH = pl.DeviceIdType.MESH
BATCHES = (3, 3, 3, 2, 1)


def round_up(value, step):
    return (value + step - 1) // step * step


def iota(shape, dim):
    return lax.broadcasted_iota(jnp.int32, shape, dim)


def nt_dot(a, b):
    return lax.dot_general(a, b, (((1,), (1,)), ((), ())), preferred_element_type=F32)


def as_column(row):
    return jnp.transpose(jnp.broadcast_to(row, (LANES, LANES)))


def lane_groups(rows):
    return [slice(g * LANES, (g + 1) * LANES) for g in range(rows // LANES)]


def kernel(
    cfg,
    h_hbm, gain_hbm, ng_hbm, kg_hbm, wb_hbm, cnt_hbm,
    hg_ref, wg_ref,
    h2, gainv, ngv, kg2, wbv, cntv,
    sq, pj, rs, nrm, onehot, onehot_t, piece_of,
    proj_early, pj_other, gathered, kept, y_send, y_recv, x_send, x_recv, zsend, zrecv, wfull, product, p_recv,
    local_sem, send_sem, sib_sem, recv_sem, by_sem, bx_sem,
):
    outer, inner, quarters, chips = cfg["outer"], cfg["inner"], cfg["quarters"], cfg["chips"]
    slots, most, group_blocks, blocks = cfg["slots"], cfg["most"], cfg["group_blocks"], cfg["blocks"]
    rows, width, pieces, model_width = cfg["rows"], cfg["width"], cfg["pieces"], cfg["model_width"]
    lane_window, row_window, padded_outer = cfg["lane_window"], cfg["row_window"], cfg["padded_outer"]
    per_group = chips * slots
    owners = outer * inner
    slot_bits = slots.bit_length() - 1
    inner_bits = inner.bit_length() - 1
    piece_bits = pieces.bit_length() - 1

    x = lax.axis_index("gx")
    y = lax.axis_index("gy")
    q = lax.axis_index("gz")
    core = lax.rem(y, CORES)
    chip = y // CORES
    other = 1 - core
    own_rows = pl.ds(pl.multiple_of(core * LANES, LANES), LANES)
    other_rows = pl.ds(pl.multiple_of(other * LANES, LANES), LANES)

    def at(gx, gchip, gcore, gz):
        return (gx, gchip * CORES + gcore, gz)

    z_peers = [(k, lax.rem(x + k, outer)) for k in range(1, outer)]
    z_peers.sort(key=lambda p: min(p[0], outer - p[0]))
    half = chips // 2
    column = lax.rem(chip, half)
    own_base = chip - column
    other_base = lax.rem(own_base + half, chips)
    across = other_base + column
    y_peer = at(x, across, core, q)
    x_peers = [(k, own_base + lax.rem(column + k, half)) for k in range(1, half)]
    SQ, C1, BY, BX, C2, PJ, ZZ = range(7)
    C1_FAR, C2_Y, C2_Y_FAR, OWN, OWN_FAR, ACROSS, ACROSS_FAR, PASS_OWN, PASS_OWN_FAR, PASS_ACROSS = range(7, 17)
    gz_peers = [
        (dc * quarters + dq - 1, lax.rem(core + dc, CORES), lax.rem(q + dq, quarters))
        for dc in range(CORES)
        for dq in range(quarters)
        if dc or dq
    ]

    offsets = sorted(range(outer), key=lambda k: -min(k, outer - k))
    place = [offsets.index(k) for k in range(outer)]
    far = sum(min(k, outer - k) > 3 for k in offsets)
    far_planes, near_planes = pl.ds(0, far), pl.ds(far, outer - far)

    loads = [
        pltpu.make_async_copy(h_hbm, h2.at[core], local_sem.at[0]),
        pltpu.make_async_copy(cnt_hbm, cntv, local_sem.at[1]),
        pltpu.make_async_copy(wb_hbm, wbv, local_sem.at[2]),
        pltpu.make_async_copy(kg_hbm, kg2.at[own_rows], local_sem.at[3]),
        pltpu.make_async_copy(gain_hbm, gainv, local_sem.at[4]),
        pltpu.make_async_copy(ng_hbm, ngv, local_sem.at[5]),
    ]
    for copy in loads:
        copy.start()
    barrier = pltpu.get_barrier_semaphore()
    peers = [at(zx, chip, core, q) for _, zx in z_peers]
    peers += [y_peer] + [at(x, to, core, q) for _, to in x_peers]
    peers += [at(x, chip, gcore, gq) for _, gcore, gq in gz_peers]
    for peer in peers:
        pl.semaphore_signal(barrier, inc=1, device_id=peer, device_id_type=MESH)

    groups = lane_groups(rows)

    loads[0].wait()
    partial = jnp.zeros((LANES, LANES), F32)
    for g in groups:
        piece = h2[core, :, g].astype(F32)
        partial = partial + piece * piece
    row = jnp.sum(jnp.transpose(partial), axis=0, keepdims=True)
    sq[core * quarters + q] = jnp.broadcast_to(row, (8, LANES))

    loads[2].wait()
    own_blocks = jnp.concatenate(
        [wbv[0, 0].astype(F32), jnp.zeros((slots - most, LANES), F32)], axis=0
    )
    gathered[chip, outer - 1] = own_blocks.astype(BF16)
    loads[3].wait()

    pl.semaphore_wait(barrier, len(peers))

    def push(src, dst, sender, receiver, peer):
        copy = pltpu.make_async_remote_copy(
            src_ref=src, dst_ref=dst, send_sem=sender, recv_sem=receiver, device_id=peer, device_id_type=MESH
        )
        copy.start()

    def arrived(like, semaphore):
        pltpu.make_async_copy(like, like, semaphore).wait()

    own_sq = sq.at[core * quarters + q]
    for _, gcore, gq in gz_peers:
        push(own_sq, own_sq, send_sem.at[SQ], recv_sem.at[SQ], at(x, chip, gcore, gq))
    own_blocks = gathered.at[chip, outer - 1]
    for k, zx in z_peers:
        spot = place[outer - k]
        push(
            own_blocks, gathered.at[chip, spot], send_sem.at[C1], recv_sem.at[C1_FAR if spot < far else C1],
            at(zx, chip, core, q),
        )
    sibling = at(x, chip, other, q)
    own_keys, own_hidden = kg2.at[own_rows], h2.at[core]
    push(own_keys, own_keys, sib_sem.at[0], sib_sem.at[1], sibling)
    push(own_hidden, own_hidden, sib_sem.at[2], sib_sem.at[3], sibling)

    loads[1].wait()
    loads[4].wait()
    counts = cntv[...].astype(F32)
    owner_of = iota((padded_outer, owners), 1)
    of_group = (owner_of >> inner_bits) == iota((padded_outer, owners), 0)
    by_group = jnp.where(of_group, jnp.broadcast_to(counts, (padded_outer, owners)), 0.0).astype(BF16)

    def placed(shape, slot_dim, owner_dim):
        slot = iota(shape, slot_dim)
        holder = (slot >> slot_bits) * CORES + core
        within = iota(shape, owner_dim) & (inner - 1)
        before = jnp.where(within < holder, 1.0, 0.0).astype(BF16)
        mine = jnp.where(within == holder, 1.0, 0.0).astype(BF16)
        return before, mine

    before, mine = placed((per_group, owners), 0, 1)
    start_c = nt_dot(before, by_group).astype(jnp.int32)
    count_c = nt_dot(mine, by_group).astype(jnp.int32)
    within_c = iota((per_group, padded_outer), 0) & (slots - 1)
    block_c = start_c + within_c + group_blocks * iota((per_group, padded_outer), 1)
    block_c = jnp.where(within_c < count_c, block_c, -pieces)
    row_c = block_c >> piece_bits
    piece_c = block_c & (pieces - 1)
    start_r = nt_dot(by_group, before).astype(jnp.int32)
    count_r = nt_dot(by_group, mine).astype(jnp.int32)
    within_r = iota((padded_outer, per_group), 1) & (slots - 1)
    block_r = start_r + within_r + group_blocks * iota((padded_outer, per_group), 0)
    block_r = jnp.where(within_r < count_r, block_r, -pieces)
    row_r = block_r >> piece_bits

    def first_lane(z):
        return group_blocks * z // pieces // LANES * LANES

    def first_row(z):
        return group_blocks * z // pieces // 8 * 8

    for z in range(outer):
        hit = row_c[:, z : z + 1] == first_lane(z) + iota((per_group, lane_window), 1)
        onehot[z] = jnp.where(hit, 1.0, 0.0).astype(BF16)
        hit = row_r[z : z + 1, :] == first_row(z) + iota((row_window, per_group), 0)
        onehot_t[z] = jnp.where(hit, 1.0, 0.0).astype(BF16)
        piece_of[z] = jnp.broadcast_to(piece_c[:, z : z + 1], (per_group, LANES))
    nrm[:, rows:] = jnp.zeros((CORES * LANES, LANES), BF16)
    wfull[...] = jnp.zeros_like(wfull)

    loads[5].wait()
    partial = jnp.zeros((LANES, LANES), F32)
    for g in groups:
        partial = partial + gainv[:, g] * ngv[:, g].astype(F32) * h2[core, :, g].astype(F32)
    proj_early[...] = partial

    def share(source, receiver, peers, planes):
        held = gathered.at[source, planes]
        for to in peers:
            push(held, held, send_sem.at[C2], recv_sem.at[receiver], at(x, to, core, q))

    along = [to for _, to in x_peers]
    ring = half == 4
    beside = [to for k, to in x_peers if not ring or k != 2]
    right, left = lax.rem(column + 1, half), lax.rem(column + half - 1, half)

    def pass_on(came_in, planes, source, receiver, to):
        if beside:
            arrived(gathered.at[pl.ds(0, len(beside)), planes], recv_sem.at[came_in])
        if ring:
            share(source, receiver, [to], planes)


    arrived(sq.at[pl.ds(0, len(gz_peers))], recv_sem.at[SQ])
    arrived(own_keys, sib_sem.at[1])
    arrived(own_hidden, sib_sem.at[3])
    for c in range(CORES):
        total = sq[c * quarters, 0:1]
        for other_q in range(1, quarters):
            total = total + sq[c * quarters + other_q, 0:1]
        rs[c] = as_column(lax.rsqrt(total / model_width + EPS))
        for g in groups:
            scaled = h2[c, :, g].astype(F32) * rs[c] * gainv[:, g]
            nrm[c * LANES : (c + 1) * LANES, g] = scaled.astype(BF16)

    ends = [sum(BATCHES[: b + 1]) for b in range(len(BATCHES))]
    spans = [(end - size, size) for end, size in zip(ends, BATCHES)]

    def slot_gradients(batch):
        start, size = spans[batch]
        for n in range(start, start + size):
            z = lax.rem(x + offsets[n], outer)
            lanes = pl.ds(pl.multiple_of(first_lane(z), LANES), lane_window)
            picked = nt_dot(onehot[z], nrm[:, lanes]).astype(BF16)
            spread = jnp.dot(picked, kg2[...], preferred_element_type=F32)
            value = spread[:, :LANES]
            for j in range(1, pieces):
                value = jnp.where(piece_of[z] == j, spread[:, j * LANES : (j + 1) * LANES], value)
            value = value.reshape(chips, slots, LANES)
            kept[:, n] = value
            y_send[:, n] = value.astype(BF16)
        span = pl.ds(start, size)
        push(
            y_send.at[pl.ds(other_base, half), span], y_recv.at[:, span], send_sem.at[BY], by_sem.at[batch], y_peer
        )

    def along_x(batch):
        start, size = spans[batch]
        span = pl.ds(start, size)
        arrived(y_recv.at[:, span], by_sem.at[batch])
        for n in range(start, start + size):
            kept[chip, n] = kept[chip, n] + y_recv[column, n].astype(F32)
            for k, to in x_peers:
                total = kept[to, n] + y_recv[to - own_base, n].astype(F32)
                x_send[k - 1, n] = total.astype(BF16)
        for k, to in x_peers:
            push(
                x_send.at[k - 1, span], x_recv.at[k - 1, span], send_sem.at[BX], bx_sem.at[batch],
                at(x, to, core, q),
            )

    def along_z(batch):
        start, size = spans[batch]
        span = pl.ds(start, size)
        if x_peers:
            arrived(x_recv.at[:, span], bx_sem.at[batch])
        for n in range(start, start + size):
            total = kept[chip, n]
            for k, _ in x_peers:
                total = total + x_recv[k - 1, n].astype(F32)
            zsend[n] = total
            if offsets[n]:
                push(
                    zsend.at[n], zrecv.at[n], send_sem.at[ZZ], recv_sem.at[ZZ],
                    at(lax.rem(x + offsets[n], outer), chip, core, q),
                )

    if outer - far > 1:
        arrived(gathered.at[chip, pl.ds(far, outer - far - 1)], recv_sem.at[C1])
    share(chip, C2_Y, [across], near_planes)
    share(chip, OWN, beside, near_planes)
    batches = range(len(BATCHES))
    for batch in batches[:1]:
        slot_gradients(batch)
    if far:
        arrived(gathered.at[chip, far_planes], recv_sem.at[C1_FAR])
        share(chip, C2_Y_FAR, [across], far_planes)
        share(chip, OWN_FAR, beside, far_planes)
    for batch in batches[1:2]:
        slot_gradients(batch)
    arrived(gathered.at[across, near_planes], recv_sem.at[C2_Y])
    share(across, ACROSS, beside, near_planes)
    pass_on(OWN, near_planes, own_base + right, PASS_OWN, own_base + left)
    for batch in batches[2:]:
        slot_gradients(batch)
    along_x(0)
    if far:
        arrived(gathered.at[across, far_planes], recv_sem.at[C2_Y_FAR])
        share(across, ACROSS_FAR, along, far_planes)
        pass_on(OWN_FAR, far_planes, own_base + left, PASS_OWN_FAR, own_base + right)
    pass_on(ACROSS, near_planes, other_base + right, PASS_ACROSS, own_base + left)
    for batch in batches[1:]:
        along_x(batch)
        if batch == 3:
            along_z(0)
    if along and far:
        arrived(gathered.at[pl.ds(0, len(along)), far_planes], recv_sem.at[ACROSS_FAR])
    if ring:
        arrived(gathered.at[0, near_planes], recv_sem.at[PASS_OWN])
        arrived(gathered.at[0, near_planes], recv_sem.at[PASS_ACROSS])
        if far:
            arrived(gathered.at[0, far_planes], recv_sem.at[PASS_OWN_FAR])
    for n in range(outer):
        z = lax.rem(x + offsets[n], outer)
        spread_rows = pl.ds(pl.multiple_of(first_row(z), 8), row_window)
        values = gathered[:, n].reshape(per_group, LANES)
        spread = jnp.concatenate(
            [jnp.where(piece_of[z] == j, values, jnp.zeros_like(values)) for j in range(pieces)], axis=1
        )
        wfull[spread_rows, :] += jnp.dot(
            onehot_t[z], spread, preferred_element_type=F32
        )
    for batch in batches[1:2]:
        along_z(batch)
    weight = wfull[:rows].astype(BF16)
    product[...] = nt_dot(kg2[...], weight)
    push(product.at[other_rows], p_recv, sib_sem.at[4], sib_sem.at[5], sibling)
    partial = proj_early[...]
    part_other = jnp.zeros((LANES, LANES), F32)
    for g in groups:
        partial = partial + gainv[:, g] * h2[core, :, g].astype(F32) * product[own_rows, g]
        part_other = part_other + gainv[:, g] * h2[other, :, g].astype(F32) * product[other_rows, g]
    own_pj = pj.at[core * quarters + q]
    pj[core * quarters + q] = jnp.broadcast_to(jnp.sum(jnp.transpose(partial), axis=0, keepdims=True), (8, LANES))
    pj_other[...] = jnp.broadcast_to(jnp.sum(jnp.transpose(part_other), axis=0, keepdims=True), (8, LANES))
    for m, gcore, gq in gz_peers:
        push(
            own_pj if m < quarters - 1 else pj_other, own_pj, send_sem.at[PJ], recv_sem.at[PJ],
            at(x, chip, gcore, gq),
        )
    for batch in [*batches[: 1 if len(batches) < 4 else 0], *batches[2:3]]:
        along_z(batch)

    arrived(p_recv, sib_sem.at[5])
    for g in groups:
        dnorm = ngv[:, g].astype(F32) + (product[own_rows, g] + p_recv[:, g])
        p_recv[:, g] = gainv[:, g] * dnorm
    for batch in batches[3:]:
        along_z(batch)
    arrived(pj.at[pl.ds(0, len(gz_peers))], recv_sem.at[PJ])
    proj = pj[0, 0:1]
    for m in range(1, CORES * quarters):
        proj = proj + pj[m, 0:1]
    rstd = rs[core]
    coefficient = rstd * rstd * rstd * as_column(proj) / model_width
    for g in groups:
        grad = p_recv[:, g] * rstd - h2[core, :, g].astype(F32) * coefficient
        hg_ref[:, g] = grad.astype(BF16)

    if z_peers:
        arrived(zrecv, recv_sem.at[ZZ])
    total = zsend[outer - 1]
    for n in range(outer - 1):
        total = total + zrecv[n]
    wg_ref[0, 0] = total[:most]
    arrived(sq.at[pl.ds(0, len(gz_peers))], send_sem.at[SQ])
    arrived(own_keys, sib_sem.at[0])
    arrived(own_hidden, sib_sem.at[2])
    arrived(p_recv, sib_sem.at[4])
    arrived(y_recv, send_sem.at[BY])
    arrived(gathered.at[pl.ds(0, chips - 1)], send_sem.at[C2])
    if x_peers:
        arrived(x_recv, send_sem.at[BX])
    if z_peers:
        arrived(gathered.at[0, pl.ds(0, outer - 1)], send_sem.at[C1])
        arrived(zrecv, send_sem.at[ZZ])
    arrived(pj.at[pl.ds(0, len(gz_peers))], send_sem.at[PJ])


def finish(most, hg_ref, wg_ref, hg_out, wg_out, lines, sem):
    wide = pltpu.make_async_copy(hg_ref, hg_out, sem.at[0])
    wide.start()
    for row in range(most):
        lines[row] = wg_ref[0, 0, row : row + 1, :]
    narrow = pltpu.make_async_copy(lines, wg_out, sem.at[1])
    narrow.start()
    wide.wait()
    narrow.wait()


def shards(hidden_in, norm_gain, normed_grad, key_grad, weight_blocks, block_count):
    outer, inner, quarters = lax.axis_size("gx"), lax.axis_size("gy"), lax.axis_size("gz")
    tokens, rows = hidden_in.shape
    width = key_grad.shape[1]
    most = weight_blocks.shape[2]
    blocks = rows * width // LANES
    pieces = width // LANES
    group_blocks = (blocks + outer - 1) // outer
    slots = round_up(most, 32)
    chips = inner // CORES
    half = chips // 2
    lines = max(half - 1, 1)
    per_group = chips * slots
    padded_outer = round_up(outer, 16)
    span = (group_blocks + pieces - 1) // pieces + 1
    cfg = dict(
        outer=outer, inner=inner, quarters=quarters, chips=chips, slots=slots, most=most,
        group_blocks=group_blocks, blocks=blocks, rows=rows, width=width, pieces=pieces,
        model_width=rows * quarters, padded_outer=padded_outer,
        lane_window=min(rows, round_up(span + LANES - 1, LANES)),
        row_window=min(rows, round_up(span + 7, 8)),
    )
    vmem = pltpu.VMEM
    dma = pltpu.SemaphoreType.DMA
    hg, wg = pl.pallas_call(
        functools.partial(kernel, cfg),
        out_shape=(
            pltpu.VMEM((tokens, rows), BF16),
            pltpu.VMEM(weight_blocks.shape, F32),
        ),
        in_specs=[pl.BlockSpec(memory_space=pltpu.HBM)] * 6,
        out_specs=(pl.BlockSpec(memory_space=pltpu.VMEM), pl.BlockSpec(memory_space=pltpu.VMEM)),
        scratch_shapes=[
            vmem((CORES, tokens, rows), BF16),
            vmem((1, rows), F32),
            vmem((tokens, rows), BF16),
            vmem((CORES * tokens, width), BF16),
            vmem(weight_blocks.shape, BF16),
            vmem(block_count.shape, jnp.int32),
            vmem((CORES * quarters, 8, LANES), F32),
            vmem((CORES * quarters, 8, LANES), F32),
            vmem((CORES, LANES, LANES), F32),
            vmem((CORES * tokens, rows + LANES), BF16),
            vmem((outer, per_group, cfg["lane_window"]), BF16),
            vmem((outer, cfg["row_window"], per_group), BF16),
            vmem((outer, per_group, LANES), jnp.int32),
            vmem((LANES, LANES), F32),
            vmem((8, LANES), F32),
            vmem((chips, outer, slots, LANES), BF16),
            vmem((chips, outer, slots, LANES), F32),
            vmem((chips, outer, slots, LANES), BF16),
            vmem((half, outer, slots, LANES), BF16),
            vmem((lines, outer, slots, LANES), BF16),
            vmem((lines, outer, slots, LANES), BF16),
            vmem((outer, slots, LANES), F32),
            vmem((max(outer - 1, 1), slots, LANES), F32),
            vmem((rows + cfg["row_window"], width), F32),
            vmem((CORES * tokens, rows), F32),
            vmem((tokens, rows), F32),
            dma((6,)), dma((7,)), dma((6,)), dma((17,)), dma((len(BATCHES),)), dma((len(BATCHES),)),
        ],
        compiler_params=pltpu.CompilerParams(
            collective_id=0, has_side_effects=True, vmem_limit_bytes=60_000_000
        ),
        name="key_projection_backward",
    )(hidden_in, norm_gain.reshape(1, rows), normed_grad, key_grad, weight_blocks, block_count)
    hg, wg = pl.pallas_call(
        functools.partial(finish, most),
        out_shape=(
            jax.ShapeDtypeStruct((tokens, rows), BF16),
            jax.ShapeDtypeStruct((most, 1, LANES), F32),
        ),
        in_specs=[pl.BlockSpec(memory_space=pltpu.VMEM)] * 2,
        out_specs=[pl.BlockSpec(memory_space=pltpu.HBM)] * 2,
        scratch_shapes=[vmem((most, 1, LANES), F32), dma((2,))],
        compiler_params=pltpu.CompilerParams(vmem_limit_bytes=2 * 1024 * 1024),
        name="write_results",
    )(hg, wg)
    return hg, wg.reshape(weight_blocks.shape)


def solution(mesh):
    placed = (
        P(("gx", "gy"), "gz"),
        P("gz"),
        P(("gx", "gy"), "gz"),
        P(("gx", "gy"), None),
        P(("gx", "gy"), "gz", None, None),
        P("gz", None),
    )
    return jax.shard_map(
        shards,
        mesh=mesh,
        in_specs=placed,
        out_specs=(P(("gx", "gy"), "gz"), P(("gx", "gy"), "gz", None, None)),
        check_vma=False,
    )
```

```python
import functools

import jax
import jax.numpy as jnp
from jax import lax
from jax.experimental import pallas as pl
from jax.experimental.pallas import tpu as pltpu
from jax.sharding import PartitionSpec as P

EPS = 1e-06
LANES = 128
CORES = 2
F32 = jnp.float32
BF16 = jnp.bfloat16
MESH = pl.DeviceIdType.MESH
BATCHES = (3, 3, 3, 2, 1)


def round_up(value, step):
    return (value + step - 1) // step * step


def iota(shape, dim):
    return lax.broadcasted_iota(jnp.int32, shape, dim)


def nt_dot(a, b):
    return lax.dot_general(a, b, (((1,), (1,)), ((), ())), preferred_element_type=F32)


def as_column(row):
    return jnp.transpose(jnp.broadcast_to(row, (LANES, LANES)))


def lane_groups(rows):
    return [slice(g * LANES, (g + 1) * LANES) for g in range(rows // LANES)]


def kernel(
    cfg,
    h_hbm, gain_hbm, ng_hbm, kg_hbm, wb_hbm, cnt_hbm,
    hg_ref, wg_ref,
    h2, gainv, ngv, kg2, wbv, cntv,
    sq, pj, rs, nrm, onehot, onehot_t, piece_of,
    proj_early, pj_other, gathered, kept, y_send, y_recv, x_send, x_recv, zsend, zrecv, wfull, product, p_recv,
    local_sem, send_sem, sib_sem, recv_sem, by_sem, bx_sem,
):
    outer, inner, quarters, chips = cfg["outer"], cfg["inner"], cfg["quarters"], cfg["chips"]
    slots, most, group_blocks, blocks = cfg["slots"], cfg["most"], cfg["group_blocks"], cfg["blocks"]
    rows, width, pieces, model_width = cfg["rows"], cfg["width"], cfg["pieces"], cfg["model_width"]
    lane_window, row_window, padded_outer = cfg["lane_window"], cfg["row_window"], cfg["padded_outer"]
    per_group = chips * slots
    owners = outer * inner
    slot_bits = slots.bit_length() - 1
    inner_bits = inner.bit_length() - 1
    piece_bits = pieces.bit_length() - 1

    x = lax.axis_index("gx")
    y = lax.axis_index("gy")
    q = lax.axis_index("gz")
    core = lax.rem(y, CORES)
    chip = y // CORES
    other = 1 - core
    own_rows = pl.ds(pl.multiple_of(core * LANES, LANES), LANES)
    other_rows = pl.ds(pl.multiple_of(other * LANES, LANES), LANES)

    def at(gx, gchip, gcore, gz):
        return (gx, gchip * CORES + gcore, gz)

    z_peers = [(k, lax.rem(x + k, outer)) for k in range(1, outer)]
    z_peers.sort(key=lambda p: min(p[0], outer - p[0]))
    half = chips // 2
    column = lax.rem(chip, half)
    own_base = chip - column
    other_base = lax.rem(own_base + half, chips)
    across = other_base + column
    y_peer = at(x, across, core, q)
    x_peers = [(k, own_base + lax.rem(column + k, half)) for k in range(1, half)]
    SQ, C1, BY, BX, C2, PJ, ZZ = range(7)
    C1_FAR, C2_Y, C2_Y_FAR, OWN, OWN_FAR, ACROSS, ACROSS_FAR, PASS_OWN, PASS_OWN_FAR, PASS_ACROSS = range(7, 17)
    gz_peers = [
        (dc * quarters + dq - 1, lax.rem(core + dc, CORES), lax.rem(q + dq, quarters))
        for dc in range(CORES)
        for dq in range(quarters)
        if dc or dq
    ]

    offsets = sorted(range(outer), key=lambda k: -min(k, outer - k))
    place = [offsets.index(k) for k in range(outer)]
    far = sum(min(k, outer - k) > 3 for k in offsets)
    far_planes, near_planes = pl.ds(0, far), pl.ds(far, outer - far)

    loads = [
        pltpu.make_async_copy(h_hbm, h2.at[core], local_sem.at[0]),
        pltpu.make_async_copy(cnt_hbm, cntv, local_sem.at[1]),
        pltpu.make_async_copy(wb_hbm, wbv, local_sem.at[2]),
        pltpu.make_async_copy(kg_hbm, kg2.at[own_rows], local_sem.at[3]),
        pltpu.make_async_copy(gain_hbm, gainv, local_sem.at[4]),
        pltpu.make_async_copy(ng_hbm, ngv, local_sem.at[5]),
    ]
    for copy in loads:
        copy.start()
    barrier = pltpu.get_barrier_semaphore()
    peers = [at(zx, chip, core, q) for _, zx in z_peers]
    peers += [y_peer] + [at(x, to, core, q) for _, to in x_peers]
    peers += [at(x, chip, gcore, gq) for _, gcore, gq in gz_peers]
    for peer in peers:
        pl.semaphore_signal(barrier, inc=1, device_id=peer, device_id_type=MESH)

    groups = lane_groups(rows)

    loads[0].wait()
    partial = jnp.zeros((LANES, LANES), F32)
    for g in groups:
        piece = h2[core, :, g].astype(F32)
        partial = partial + piece * piece
    row = jnp.sum(jnp.transpose(partial), axis=0, keepdims=True)
    sq[core * quarters + q] = jnp.broadcast_to(row, (8, LANES))

    loads[2].wait()
    own_blocks = jnp.concatenate(
        [wbv[0, 0].astype(F32), jnp.zeros((slots - most, LANES), F32)], axis=0
    )
    gathered[chip, outer - 1] = own_blocks.astype(BF16)
    loads[3].wait()

    pl.semaphore_wait(barrier, len(peers))

    def push(src, dst, sender, receiver, peer):
        copy = pltpu.make_async_remote_copy(
            src_ref=src, dst_ref=dst, send_sem=sender, recv_sem=receiver, device_id=peer, device_id_type=MESH
        )
        copy.start()

    def arrived(like, semaphore):
        pltpu.make_async_copy(like, like, semaphore).wait()

    own_sq = sq.at[core * quarters + q]
    for _, gcore, gq in gz_peers:
        push(own_sq, own_sq, send_sem.at[SQ], recv_sem.at[SQ], at(x, chip, gcore, gq))
    own_blocks = gathered.at[chip, outer - 1]
    for k, zx in z_peers:
        spot = place[outer - k]
        push(
            own_blocks, gathered.at[chip, spot], send_sem.at[C1], recv_sem.at[C1_FAR if spot < far else C1],
            at(zx, chip, core, q),
        )
    sibling = at(x, chip, other, q)
    own_keys, own_hidden = kg2.at[own_rows], h2.at[core]
    push(own_keys, own_keys, sib_sem.at[0], sib_sem.at[1], sibling)
    push(own_hidden, own_hidden, sib_sem.at[2], sib_sem.at[3], sibling)

    loads[1].wait()
    loads[4].wait()
    counts = cntv[...].astype(F32)
    owner_of = iota((padded_outer, owners), 1)
    of_group = (owner_of >> inner_bits) == iota((padded_outer, owners), 0)
    by_group = jnp.where(of_group, jnp.broadcast_to(counts, (padded_outer, owners)), 0.0).astype(BF16)

    def placed(shape, slot_dim, owner_dim):
        slot = iota(shape, slot_dim)
        holder = (slot >> slot_bits) * CORES + core
        within = iota(shape, owner_dim) & (inner - 1)
        before = jnp.where(within < holder, 1.0, 0.0).astype(BF16)
        mine = jnp.where(within == holder, 1.0, 0.0).astype(BF16)
        return before, mine

    before, mine = placed((per_group, owners), 0, 1)
    start_c = nt_dot(before, by_group).astype(jnp.int32)
    count_c = nt_dot(mine, by_group).astype(jnp.int32)
    within_c = iota((per_group, padded_outer), 0) & (slots - 1)
    block_c = start_c + within_c + group_blocks * iota((per_group, padded_outer), 1)
    block_c = jnp.where(within_c < count_c, block_c, -pieces)
    row_c = block_c >> piece_bits
    piece_c = block_c & (pieces - 1)
    start_r = nt_dot(by_group, before).astype(jnp.int32)
    count_r = nt_dot(by_group, mine).astype(jnp.int32)
    within_r = iota((padded_outer, per_group), 1) & (slots - 1)
    block_r = start_r + within_r + group_blocks * iota((padded_outer, per_group), 0)
    block_r = jnp.where(within_r < count_r, block_r, -pieces)
    row_r = block_r >> piece_bits

    def first_lane(z):
        return group_blocks * z // pieces // LANES * LANES

    def first_row(z):
        return group_blocks * z // pieces // 8 * 8

    for z in range(outer):
        hit = row_c[:, z : z + 1] == first_lane(z) + iota((per_group, lane_window), 1)
        onehot[z] = jnp.where(hit, 1.0, 0.0).astype(BF16)
        hit = row_r[z : z + 1, :] == first_row(z) + iota((row_window, per_group), 0)
        onehot_t[z] = jnp.where(hit, 1.0, 0.0).astype(BF16)
        piece_of[z] = jnp.broadcast_to(piece_c[:, z : z + 1], (per_group, LANES))
    nrm[:, rows:] = jnp.zeros((CORES * LANES, LANES), BF16)
    wfull[...] = jnp.zeros_like(wfull)

    loads[5].wait()
    partial = jnp.zeros((LANES, LANES), F32)
    for g in groups:
        partial = partial + gainv[:, g] * ngv[:, g].astype(F32) * h2[core, :, g].astype(F32)
    proj_early[...] = partial

    def share(source, receiver, peers, planes):
        held = gathered.at[source, planes]
        for to in peers:
            push(held, held, send_sem.at[C2], recv_sem.at[receiver], at(x, to, core, q))

    along = [to for _, to in x_peers]
    ring = half == 4
    beside = [to for k, to in x_peers if not ring or k != 2]
    right, left = lax.rem(column + 1, half), lax.rem(column + half - 1, half)

    def pass_on(came_in, planes, source, receiver, to):
        if beside:
            arrived(gathered.at[pl.ds(0, len(beside)), planes], recv_sem.at[came_in])
        if ring:
            share(source, receiver, [to], planes)


    if outer - far > 1:
        arrived(gathered.at[chip, pl.ds(far, outer - far - 1)], recv_sem.at[C1])
    share(chip, C2_Y, [across], near_planes)
    share(chip, OWN, beside, near_planes)
    arrived(sq.at[pl.ds(0, len(gz_peers))], recv_sem.at[SQ])
    arrived(own_keys, sib_sem.at[1])
    arrived(own_hidden, sib_sem.at[3])
    for c in range(CORES):
        total = sq[c * quarters, 0:1]
        for other_q in range(1, quarters):
            total = total + sq[c * quarters + other_q, 0:1]
        rs[c] = as_column(lax.rsqrt(total / model_width + EPS))
        for g in groups:
            scaled = h2[c, :, g].astype(F32) * rs[c] * gainv[:, g]
            nrm[c * LANES : (c + 1) * LANES, g] = scaled.astype(BF16)

    ends = [sum(BATCHES[: b + 1]) for b in range(len(BATCHES))]
    spans = [(end - size, size) for end, size in zip(ends, BATCHES)]

    def slot_gradients(batch):
        start, size = spans[batch]
        for n in range(start, start + size):
            z = lax.rem(x + offsets[n], outer)
            lanes = pl.ds(pl.multiple_of(first_lane(z), LANES), lane_window)
            picked = nt_dot(onehot[z], nrm[:, lanes]).astype(BF16)
            spread = jnp.dot(picked, kg2[...], preferred_element_type=F32)
            value = spread[:, :LANES]
            for j in range(1, pieces):
                value = jnp.where(piece_of[z] == j, spread[:, j * LANES : (j + 1) * LANES], value)
            value = value.reshape(chips, slots, LANES)
            kept[:, n] = value
            y_send[:, n] = value.astype(BF16)
        span = pl.ds(start, size)
        push(
            y_send.at[pl.ds(other_base, half), span], y_recv.at[:, span], send_sem.at[BY], by_sem.at[batch], y_peer
        )

    def along_x(batch):
        start, size = spans[batch]
        span = pl.ds(start, size)
        arrived(y_recv.at[:, span], by_sem.at[batch])
        for n in range(start, start + size):
            kept[chip, n] = kept[chip, n] + y_recv[column, n].astype(F32)
            for k, to in x_peers:
                total = kept[to, n] + y_recv[to - own_base, n].astype(F32)
                x_send[k - 1, n] = total.astype(BF16)
        for k, to in x_peers:
            push(
                x_send.at[k - 1, span], x_recv.at[k - 1, span], send_sem.at[BX], bx_sem.at[batch],
                at(x, to, core, q),
            )

    def along_z(batch):
        start, size = spans[batch]
        span = pl.ds(start, size)
        if x_peers:
            arrived(x_recv.at[:, span], bx_sem.at[batch])
        for n in range(start, start + size):
            total = kept[chip, n]
            for k, _ in x_peers:
                total = total + x_recv[k - 1, n].astype(F32)
            zsend[n] = total
            if offsets[n]:
                push(
                    zsend.at[n], zrecv.at[n], send_sem.at[ZZ], recv_sem.at[ZZ],
                    at(lax.rem(x + offsets[n], outer), chip, core, q),
                )

    batches = range(len(BATCHES))
    for batch in batches[:1]:
        slot_gradients(batch)
    if far:
        arrived(gathered.at[chip, far_planes], recv_sem.at[C1_FAR])
        share(chip, C2_Y_FAR, [across], far_planes)
        share(chip, OWN_FAR, beside, far_planes)
    for batch in batches[1:2]:
        slot_gradients(batch)
    arrived(gathered.at[across, near_planes], recv_sem.at[C2_Y])
    share(across, ACROSS, beside, near_planes)
    pass_on(OWN, near_planes, own_base + right, PASS_OWN, own_base + left)
    for batch in batches[2:]:
        slot_gradients(batch)
    along_x(0)
    if far:
        arrived(gathered.at[across, far_planes], recv_sem.at[C2_Y_FAR])
        share(across, ACROSS_FAR, along, far_planes)
        pass_on(OWN_FAR, far_planes, own_base + left, PASS_OWN_FAR, own_base + right)
    pass_on(ACROSS, near_planes, other_base + right, PASS_ACROSS, own_base + left)
    def weight_rows(planes):
        for n in planes:
            z = lax.rem(x + offsets[n], outer)
            spread_rows = pl.ds(pl.multiple_of(first_row(z), 8), row_window)
            values = gathered[:, n].reshape(per_group, LANES)
            spread = jnp.concatenate(
                [jnp.where(piece_of[z] == j, values, jnp.zeros_like(values)) for j in range(pieces)], axis=1
            )
            wfull[spread_rows, :] += jnp.dot(onehot_t[z], spread, preferred_element_type=F32)

    for batch in batches[1:]:
        along_x(batch)
        if batch == 3:
            along_z(0)
            if far:
                arrived(gathered.at[pl.ds(0, len(along)), far_planes], recv_sem.at[ACROSS_FAR])
                arrived(gathered.at[0, far_planes], recv_sem.at[PASS_OWN_FAR])
            weight_rows(range(far))
    if ring:
        arrived(gathered.at[0, near_planes], recv_sem.at[PASS_OWN])
        arrived(gathered.at[0, near_planes], recv_sem.at[PASS_ACROSS])
    weight_rows(range(far, outer))
    for batch in batches[1:2]:
        along_z(batch)
    weight = wfull[:rows].astype(BF16)
    product[...] = nt_dot(kg2[...], weight)
    push(product.at[other_rows], p_recv, sib_sem.at[4], sib_sem.at[5], sibling)
    partial = proj_early[...]
    part_other = jnp.zeros((LANES, LANES), F32)
    for g in groups:
        partial = partial + gainv[:, g] * h2[core, :, g].astype(F32) * product[own_rows, g]
        part_other = part_other + gainv[:, g] * h2[other, :, g].astype(F32) * product[other_rows, g]
    own_pj = pj.at[core * quarters + q]
    pj[core * quarters + q] = jnp.broadcast_to(jnp.sum(jnp.transpose(partial), axis=0, keepdims=True), (8, LANES))
    pj_other[...] = jnp.broadcast_to(jnp.sum(jnp.transpose(part_other), axis=0, keepdims=True), (8, LANES))
    for m, gcore, gq in gz_peers:
        push(
            own_pj if m < quarters - 1 else pj_other, own_pj, send_sem.at[PJ], recv_sem.at[PJ],
            at(x, chip, gcore, gq),
        )
    for batch in [*batches[: 1 if len(batches) < 4 else 0], *batches[2:3]]:
        along_z(batch)

    arrived(p_recv, sib_sem.at[5])
    for g in groups:
        dnorm = ngv[:, g].astype(F32) + (product[own_rows, g] + p_recv[:, g])
        p_recv[:, g] = gainv[:, g] * dnorm
    for batch in batches[3:]:
        along_z(batch)
    arrived(pj.at[pl.ds(0, len(gz_peers))], recv_sem.at[PJ])
    proj = pj[0, 0:1]
    for m in range(1, CORES * quarters):
        proj = proj + pj[m, 0:1]
    rstd = rs[core]
    coefficient = rstd * rstd * rstd * as_column(proj) / model_width
    for g in groups:
        grad = p_recv[:, g] * rstd - h2[core, :, g].astype(F32) * coefficient
        hg_ref[:, g] = grad.astype(BF16)

    if z_peers:
        arrived(zrecv, recv_sem.at[ZZ])
    total = zsend[outer - 1]
    for n in range(outer - 1):
        total = total + zrecv[n]
    wg_ref[0, 0] = total[:most]
    arrived(sq.at[pl.ds(0, len(gz_peers))], send_sem.at[SQ])
    arrived(own_keys, sib_sem.at[0])
    arrived(own_hidden, sib_sem.at[2])
    arrived(p_recv, sib_sem.at[4])
    arrived(y_recv, send_sem.at[BY])
    arrived(gathered.at[pl.ds(0, chips - 1)], send_sem.at[C2])
    if x_peers:
        arrived(x_recv, send_sem.at[BX])
    if z_peers:
        arrived(gathered.at[0, pl.ds(0, outer - 1)], send_sem.at[C1])
        arrived(zrecv, send_sem.at[ZZ])
    arrived(pj.at[pl.ds(0, len(gz_peers))], send_sem.at[PJ])


def finish(most, hg_ref, wg_ref, hg_out, wg_out, lines, sem):
    wide = pltpu.make_async_copy(hg_ref, hg_out, sem.at[0])
    wide.start()
    for row in range(most):
        lines[row] = wg_ref[0, 0, row : row + 1, :]
    narrow = pltpu.make_async_copy(lines, wg_out, sem.at[1])
    narrow.start()
    wide.wait()
    narrow.wait()


def shards(hidden_in, norm_gain, normed_grad, key_grad, weight_blocks, block_count):
    outer, inner, quarters = lax.axis_size("gx"), lax.axis_size("gy"), lax.axis_size("gz")
    tokens, rows = hidden_in.shape
    width = key_grad.shape[1]
    most = weight_blocks.shape[2]
    blocks = rows * width // LANES
    pieces = width // LANES
    group_blocks = (blocks + outer - 1) // outer
    slots = round_up(most, 32)
    chips = inner // CORES
    half = chips // 2
    lines = max(half - 1, 1)
    per_group = chips * slots
    padded_outer = round_up(outer, 16)
    span = (group_blocks + pieces - 1) // pieces + 1
    cfg = dict(
        outer=outer, inner=inner, quarters=quarters, chips=chips, slots=slots, most=most,
        group_blocks=group_blocks, blocks=blocks, rows=rows, width=width, pieces=pieces,
        model_width=rows * quarters, padded_outer=padded_outer,
        lane_window=min(rows, round_up(span + LANES - 1, LANES)),
        row_window=min(rows, round_up(span + 7, 8)),
    )
    vmem = pltpu.VMEM
    dma = pltpu.SemaphoreType.DMA
    hg, wg = pl.pallas_call(
        functools.partial(kernel, cfg),
        out_shape=(
            pltpu.VMEM((tokens, rows), BF16),
            pltpu.VMEM(weight_blocks.shape, F32),
        ),
        in_specs=[pl.BlockSpec(memory_space=pltpu.HBM)] * 6,
        out_specs=(pl.BlockSpec(memory_space=pltpu.VMEM), pl.BlockSpec(memory_space=pltpu.VMEM)),
        scratch_shapes=[
            vmem((CORES, tokens, rows), BF16),
            vmem((1, rows), F32),
            vmem((tokens, rows), BF16),
            vmem((CORES * tokens, width), BF16),
            vmem(weight_blocks.shape, BF16),
            vmem(block_count.shape, jnp.int32),
            vmem((CORES * quarters, 8, LANES), F32),
            vmem((CORES * quarters, 8, LANES), F32),
            vmem((CORES, LANES, LANES), F32),
            vmem((CORES * tokens, rows + LANES), BF16),
            vmem((outer, per_group, cfg["lane_window"]), BF16),
            vmem((outer, cfg["row_window"], per_group), BF16),
            vmem((outer, per_group, LANES), jnp.int32),
            vmem((LANES, LANES), F32),
            vmem((8, LANES), F32),
            vmem((chips, outer, slots, LANES), BF16),
            vmem((chips, outer, slots, LANES), F32),
            vmem((chips, outer, slots, LANES), BF16),
            vmem((half, outer, slots, LANES), BF16),
            vmem((lines, outer, slots, LANES), BF16),
            vmem((lines, outer, slots, LANES), BF16),
            vmem((outer, slots, LANES), F32),
            vmem((max(outer - 1, 1), slots, LANES), F32),
            vmem((rows + cfg["row_window"], width), F32),
            vmem((CORES * tokens, rows), F32),
            vmem((tokens, rows), F32),
            dma((6,)), dma((7,)), dma((6,)), dma((17,)), dma((len(BATCHES),)), dma((len(BATCHES),)),
        ],
        compiler_params=pltpu.CompilerParams(
            collective_id=0, has_side_effects=True, vmem_limit_bytes=60_000_000
        ),
        name="key_projection_backward",
    )(hidden_in, norm_gain.reshape(1, rows), normed_grad, key_grad, weight_blocks, block_count)
    hg, wg = pl.pallas_call(
        functools.partial(finish, most),
        out_shape=(
            jax.ShapeDtypeStruct((tokens, rows), BF16),
            jax.ShapeDtypeStruct((most, 1, LANES), F32),
        ),
        in_specs=[pl.BlockSpec(memory_space=pltpu.VMEM)] * 2,
        out_specs=[pl.BlockSpec(memory_space=pltpu.HBM)] * 2,
        scratch_shapes=[vmem((most, 1, LANES), F32), dma((2,))],
        compiler_params=pltpu.CompilerParams(vmem_limit_bytes=2 * 1024 * 1024),
        name="write_results",
    )(hg, wg)
    return hg, wg.reshape(weight_blocks.shape)


def solution(mesh):
    placed = (
        P(("gx", "gy"), "gz"),
        P("gz"),
        P(("gx", "gy"), "gz"),
        P(("gx", "gy"), None),
        P(("gx", "gy"), "gz", None, None),
        P("gz", None),
    )
    return jax.shard_map(
        shards,
        mesh=mesh,
        in_specs=placed,
        out_specs=(P(("gx", "gy"), "gz"), P(("gx", "gy"), "gz", None, None)),
        check_vma=False,
    )
```

```python
import functools

import jax
import jax.numpy as jnp
from jax import lax
from jax.experimental import pallas as pl
from jax.experimental.pallas import tpu as pltpu
from jax.sharding import PartitionSpec as P

EPS = 1e-06
LANES = 128
CORES = 2
F32 = jnp.float32
BF16 = jnp.bfloat16
MESH = pl.DeviceIdType.MESH
BATCHES = (3, 3, 3, 2, 1)


def round_up(value, step):
    return (value + step - 1) // step * step


def iota(shape, dim):
    return lax.broadcasted_iota(jnp.int32, shape, dim)


def nt_dot(a, b):
    return lax.dot_general(a, b, (((1,), (1,)), ((), ())), preferred_element_type=F32)


def as_column(row):
    return jnp.transpose(jnp.broadcast_to(row, (LANES, LANES)))


def lane_groups(rows):
    return [slice(g * LANES, (g + 1) * LANES) for g in range(rows // LANES)]


def kernel(
    cfg,
    h_hbm, gain_hbm, ng_hbm, kg_hbm, wb_hbm, cnt_hbm,
    hg_ref, wg_ref,
    h2, gainv, ngv, kg2, wbv, cntv,
    sq, pj, rs, nrm, onehot, onehot_t, piece_of,
    proj_early, pj_other, gathered, kept, y_send, y_recv, x_send, x_recv, zsend, zrecv, wfull, product, p_recv,
    local_sem, send_sem, sib_sem, recv_sem, by_sem, bx_sem,
):
    outer, inner, quarters, chips = cfg["outer"], cfg["inner"], cfg["quarters"], cfg["chips"]
    slots, most, group_blocks, blocks = cfg["slots"], cfg["most"], cfg["group_blocks"], cfg["blocks"]
    rows, width, pieces, model_width = cfg["rows"], cfg["width"], cfg["pieces"], cfg["model_width"]
    lane_window, row_window, padded_outer = cfg["lane_window"], cfg["row_window"], cfg["padded_outer"]
    per_group = chips * slots
    owners = outer * inner
    slot_bits = slots.bit_length() - 1
    inner_bits = inner.bit_length() - 1
    piece_bits = pieces.bit_length() - 1

    x = lax.axis_index("gx")
    y = lax.axis_index("gy")
    q = lax.axis_index("gz")
    core = lax.rem(y, CORES)
    chip = y // CORES
    other = 1 - core
    own_rows = pl.ds(pl.multiple_of(core * LANES, LANES), LANES)
    other_rows = pl.ds(pl.multiple_of(other * LANES, LANES), LANES)

    def at(gx, gchip, gcore, gz):
        return (gx, gchip * CORES + gcore, gz)

    z_peers = [(k, lax.rem(x + k, outer)) for k in range(1, outer)]
    z_peers.sort(key=lambda p: min(p[0], outer - p[0]))
    half = chips // 2
    column = lax.rem(chip, half)
    own_base = chip - column
    other_base = lax.rem(own_base + half, chips)
    across = other_base + column
    y_peer = at(x, across, core, q)
    x_peers = [(k, own_base + lax.rem(column + k, half)) for k in range(1, half)]
    SQ, C1, BY, BX, C2, PJ, ZZ = range(7)
    C1_FAR, C2_Y, C2_Y_FAR, OWN, OWN_FAR, ACROSS, ACROSS_FAR, PASS_OWN, PASS_OWN_FAR, PASS_ACROSS = range(7, 17)
    gz_peers = [
        (dc * quarters + dq - 1, lax.rem(core + dc, CORES), lax.rem(q + dq, quarters))
        for dc in range(CORES)
        for dq in range(quarters)
        if dc or dq
    ]

    offsets = sorted(range(outer), key=lambda k: -min(k, outer - k))
    place = [offsets.index(k) for k in range(outer)]
    far = sum(min(k, outer - k) > 3 for k in offsets)
    far_planes, near_planes = pl.ds(0, far), pl.ds(far, outer - far)

    loads = [
        pltpu.make_async_copy(h_hbm, h2.at[core], local_sem.at[0]),
        pltpu.make_async_copy(cnt_hbm, cntv, local_sem.at[1]),
        pltpu.make_async_copy(wb_hbm, wbv, local_sem.at[2]),
        pltpu.make_async_copy(kg_hbm, kg2.at[own_rows], local_sem.at[3]),
        pltpu.make_async_copy(gain_hbm, gainv, local_sem.at[4]),
        pltpu.make_async_copy(ng_hbm, ngv, local_sem.at[5]),
    ]
    for copy in loads:
        copy.start()
    barrier = pltpu.get_barrier_semaphore()
    peers = [at(zx, chip, core, q) for _, zx in z_peers]
    peers += [y_peer] + [at(x, to, core, q) for _, to in x_peers]
    peers += [at(x, chip, gcore, gq) for _, gcore, gq in gz_peers]
    for peer in peers:
        pl.semaphore_signal(barrier, inc=1, device_id=peer, device_id_type=MESH)

    groups = lane_groups(rows)

    loads[0].wait()
    partial = jnp.zeros((LANES, LANES), F32)
    for g in groups:
        piece = h2[core, :, g].astype(F32)
        partial = partial + piece * piece
    row = jnp.sum(jnp.transpose(partial), axis=0, keepdims=True)
    sq[core * quarters + q] = jnp.broadcast_to(row, (8, LANES))

    loads[2].wait()
    own_blocks = jnp.concatenate(
        [wbv[0, 0].astype(F32), jnp.zeros((slots - most, LANES), F32)], axis=0
    )
    gathered[chip, outer - 1] = own_blocks.astype(BF16)
    loads[3].wait()

    pl.semaphore_wait(barrier, len(peers))

    def push(src, dst, sender, receiver, peer):
        copy = pltpu.make_async_remote_copy(
            src_ref=src, dst_ref=dst, send_sem=sender, recv_sem=receiver, device_id=peer, device_id_type=MESH
        )
        copy.start()

    def arrived(like, semaphore):
        pltpu.make_async_copy(like, like, semaphore).wait()

    own_sq = sq.at[core * quarters + q]
    for _, gcore, gq in gz_peers:
        push(own_sq, own_sq, send_sem.at[SQ], recv_sem.at[SQ], at(x, chip, gcore, gq))
    own_blocks = gathered.at[chip, outer - 1]
    for k, zx in z_peers:
        spot = place[outer - k]
        push(
            own_blocks, gathered.at[chip, spot], send_sem.at[C1], recv_sem.at[C1_FAR if spot < far else C1],
            at(zx, chip, core, q),
        )
    sibling = at(x, chip, other, q)
    own_keys, own_hidden = kg2.at[own_rows], h2.at[core]
    push(own_keys, own_keys, sib_sem.at[0], sib_sem.at[1], sibling)
    push(own_hidden, own_hidden, sib_sem.at[2], sib_sem.at[3], sibling)

    loads[1].wait()
    loads[4].wait()
    counts = cntv[...].astype(F32)
    owner_of = iota((padded_outer, owners), 1)
    of_group = (owner_of >> inner_bits) == iota((padded_outer, owners), 0)
    by_group = jnp.where(of_group, jnp.broadcast_to(counts, (padded_outer, owners)), 0.0).astype(BF16)

    def placed(shape, slot_dim, owner_dim):
        slot = iota(shape, slot_dim)
        holder = (slot >> slot_bits) * CORES + core
        within = iota(shape, owner_dim) & (inner - 1)
        before = jnp.where(within < holder, 1.0, 0.0).astype(BF16)
        mine = jnp.where(within == holder, 1.0, 0.0).astype(BF16)
        return before, mine

    before, mine = placed((per_group, owners), 0, 1)
    start_c = nt_dot(before, by_group).astype(jnp.int32)
    count_c = nt_dot(mine, by_group).astype(jnp.int32)
    within_c = iota((per_group, padded_outer), 0) & (slots - 1)
    block_c = start_c + within_c + group_blocks * iota((per_group, padded_outer), 1)
    block_c = jnp.where(within_c < count_c, block_c, -pieces)
    row_c = block_c >> piece_bits
    piece_c = block_c & (pieces - 1)
    start_r = nt_dot(by_group, before).astype(jnp.int32)
    count_r = nt_dot(by_group, mine).astype(jnp.int32)
    within_r = iota((padded_outer, per_group), 1) & (slots - 1)
    block_r = start_r + within_r + group_blocks * iota((padded_outer, per_group), 0)
    block_r = jnp.where(within_r < count_r, block_r, -pieces)
    row_r = block_r >> piece_bits

    def first_lane(z):
        return group_blocks * z // pieces // LANES * LANES

    def first_row(z):
        return group_blocks * z // pieces // 8 * 8

    for z in range(outer):
        hit = row_c[:, z : z + 1] == first_lane(z) + iota((per_group, lane_window), 1)
        onehot[z] = jnp.where(hit, 1.0, 0.0).astype(BF16)
        hit = row_r[z : z + 1, :] == first_row(z) + iota((row_window, per_group), 0)
        onehot_t[z] = jnp.where(hit, 1.0, 0.0).astype(BF16)
        piece_of[z] = jnp.broadcast_to(piece_c[:, z : z + 1], (per_group, LANES))
    nrm[:, rows:] = jnp.zeros((CORES * LANES, LANES), BF16)
    wfull[...] = jnp.zeros_like(wfull)

    loads[5].wait()
    partial = jnp.zeros((LANES, LANES), F32)
    for g in groups:
        partial = partial + gainv[:, g] * ngv[:, g].astype(F32) * h2[core, :, g].astype(F32)
    proj_early[...] = partial

    def share(source, receiver, peers, planes):
        held = gathered.at[source, planes]
        for to in peers:
            push(held, held, send_sem.at[C2], recv_sem.at[receiver], at(x, to, core, q))

    along = [to for _, to in x_peers]
    ring = half == 4
    beside = [to for k, to in x_peers if not ring or k != 2]
    right, left = lax.rem(column + 1, half), lax.rem(column + half - 1, half)

    def pass_on(came_in, planes, source, receiver, to):
        if beside:
            arrived(gathered.at[pl.ds(0, len(beside)), planes], recv_sem.at[came_in])
        if ring:
            share(source, receiver, [to], planes)


    if outer - far > 1:
        arrived(gathered.at[chip, pl.ds(far, outer - far - 1)], recv_sem.at[C1])
    share(chip, C2_Y, [across], near_planes)
    share(chip, OWN, beside, near_planes)
    arrived(sq.at[pl.ds(0, len(gz_peers))], recv_sem.at[SQ])
    arrived(own_keys, sib_sem.at[1])
    arrived(own_hidden, sib_sem.at[3])
    for c in range(CORES):
        total = sq[c * quarters, 0:1]
        for other_q in range(1, quarters):
            total = total + sq[c * quarters + other_q, 0:1]
        rs[c] = as_column(lax.rsqrt(total / model_width + EPS))
        for g in groups:
            scaled = h2[c, :, g].astype(F32) * rs[c] * gainv[:, g]
            nrm[c * LANES : (c + 1) * LANES, g] = scaled.astype(BF16)

    ends = [sum(BATCHES[: b + 1]) for b in range(len(BATCHES))]
    spans = [(end - size, size) for end, size in zip(ends, BATCHES)]

    def slot_gradients(batch):
        start, size = spans[batch]
        for n in range(start, start + size):
            z = lax.rem(x + offsets[n], outer)
            lanes = pl.ds(pl.multiple_of(first_lane(z), LANES), lane_window)
            picked = nt_dot(onehot[z], nrm[:, lanes]).astype(BF16)
            spread = jnp.dot(picked, kg2[...], preferred_element_type=F32)
            value = spread[:, :LANES]
            for j in range(1, pieces):
                value = jnp.where(piece_of[z] == j, spread[:, j * LANES : (j + 1) * LANES], value)
            value = value.reshape(chips, slots, LANES)
            kept[:, n] = value
            y_send[:, n] = value.astype(BF16)
        span = pl.ds(start, size)
        push(
            y_send.at[pl.ds(other_base, half), span], y_recv.at[:, span], send_sem.at[BY], by_sem.at[batch], y_peer
        )

    def along_x(batch):
        start, size = spans[batch]
        span = pl.ds(start, size)
        arrived(y_recv.at[:, span], by_sem.at[batch])
        for n in range(start, start + size):
            kept[chip, n] = kept[chip, n] + y_recv[column, n].astype(F32)
            for k, to in x_peers:
                total = kept[to, n] + y_recv[to - own_base, n].astype(F32)
                x_send[k - 1, n] = total.astype(BF16)
        for k, to in x_peers:
            push(
                x_send.at[k - 1, span], x_recv.at[k - 1, span], send_sem.at[BX], bx_sem.at[batch],
                at(x, to, core, q),
            )

    def along_z(batch):
        start, size = spans[batch]
        span = pl.ds(start, size)
        if x_peers:
            arrived(x_recv.at[:, span], bx_sem.at[batch])
        for n in range(start, start + size):
            total = kept[chip, n]
            for k, _ in x_peers:
                total = total + x_recv[k - 1, n].astype(F32)
            zsend[n] = total
            if offsets[n]:
                push(
                    zsend.at[n], zrecv.at[n], send_sem.at[ZZ], recv_sem.at[ZZ],
                    at(lax.rem(x + offsets[n], outer), chip, core, q),
                )

    batches = range(len(BATCHES))
    for batch in batches[:1]:
        slot_gradients(batch)
    if far:
        arrived(gathered.at[chip, far_planes], recv_sem.at[C1_FAR])
        share(chip, C2_Y_FAR, [across], far_planes)
        share(chip, OWN_FAR, beside, far_planes)
    for batch in batches[1:2]:
        slot_gradients(batch)
    arrived(gathered.at[across, near_planes], recv_sem.at[C2_Y])
    share(across, ACROSS, beside, near_planes)
    pass_on(OWN, near_planes, own_base + right, PASS_OWN, own_base + left)
    for batch in batches[2:]:
        slot_gradients(batch)
    along_x(0)
    if far:
        arrived(gathered.at[across, far_planes], recv_sem.at[C2_Y_FAR])
        share(across, ACROSS_FAR, along, far_planes)
        pass_on(OWN_FAR, far_planes, own_base + left, PASS_OWN_FAR, own_base + right)
    pass_on(ACROSS, near_planes, other_base + right, PASS_ACROSS, own_base + left)
    def weight_rows(planes):
        for n in planes:
            z = lax.rem(x + offsets[n], outer)
            spread_rows = pl.ds(pl.multiple_of(first_row(z), 8), row_window)
            values = gathered[:, n].reshape(per_group, LANES)
            spread = jnp.concatenate(
                [jnp.where(piece_of[z] == j, values, jnp.zeros_like(values)) for j in range(pieces)], axis=1
            )
            wfull[spread_rows, :] += jnp.dot(onehot_t[z], spread, preferred_element_type=F32)

    for batch in batches[1:]:
        along_x(batch)
        if batch == 3:
            along_z(0)
            if far:
                arrived(gathered.at[pl.ds(0, len(along)), far_planes], recv_sem.at[ACROSS_FAR])
                arrived(gathered.at[0, far_planes], recv_sem.at[PASS_OWN_FAR])
            weight_rows(range(far))
    if ring:
        arrived(gathered.at[0, near_planes], recv_sem.at[PASS_OWN])
        arrived(gathered.at[0, near_planes], recv_sem.at[PASS_ACROSS])
    weight_rows(range(far, outer))
    for batch in batches[1:2]:
        along_z(batch)
    weight = wfull[:rows].astype(BF16)
    product[...] = nt_dot(kg2[...], weight)
    partial = proj_early[...]
    part_other = jnp.zeros((LANES, LANES), F32)
    for g in groups:
        partial = partial + gainv[:, g] * h2[core, :, g].astype(F32) * product[own_rows, g]
        part_other = part_other + gainv[:, g] * h2[other, :, g].astype(F32) * product[other_rows, g]
    own_pj = pj.at[core * quarters + q]
    pj[core * quarters + q] = jnp.broadcast_to(jnp.sum(jnp.transpose(partial), axis=0, keepdims=True), (8, LANES))
    pj_other[...] = jnp.broadcast_to(jnp.sum(jnp.transpose(part_other), axis=0, keepdims=True), (8, LANES))
    for m, gcore, gq in gz_peers:
        push(
            own_pj if m < quarters - 1 else pj_other, own_pj, send_sem.at[PJ], recv_sem.at[PJ],
            at(x, chip, gcore, gq),
        )
    push(product.at[other_rows], p_recv, sib_sem.at[4], sib_sem.at[5], sibling)
    for batch in [*batches[: 1 if len(batches) < 4 else 0], *batches[2:3]]:
        along_z(batch)

    arrived(p_recv, sib_sem.at[5])
    for g in groups:
        dnorm = ngv[:, g].astype(F32) + (product[own_rows, g] + p_recv[:, g])
        p_recv[:, g] = gainv[:, g] * dnorm
    for batch in batches[3:]:
        along_z(batch)
    arrived(pj.at[pl.ds(0, len(gz_peers))], recv_sem.at[PJ])
    proj = pj[0, 0:1]
    for m in range(1, CORES * quarters):
        proj = proj + pj[m, 0:1]
    rstd = rs[core]
    coefficient = rstd * rstd * rstd * as_column(proj) / model_width
    for g in groups:
        grad = p_recv[:, g] * rstd - h2[core, :, g].astype(F32) * coefficient
        hg_ref[:, g] = grad.astype(BF16)

    if z_peers:
        arrived(zrecv, recv_sem.at[ZZ])
    total = zsend[outer - 1]
    for n in range(outer - 1):
        total = total + zrecv[n]
    wg_ref[0, 0] = total[:most]
    arrived(sq.at[pl.ds(0, len(gz_peers))], send_sem.at[SQ])
    arrived(own_keys, sib_sem.at[0])
    arrived(own_hidden, sib_sem.at[2])
    arrived(p_recv, sib_sem.at[4])
    arrived(y_recv, send_sem.at[BY])
    arrived(gathered.at[pl.ds(0, chips - 1)], send_sem.at[C2])
    if x_peers:
        arrived(x_recv, send_sem.at[BX])
    if z_peers:
        arrived(gathered.at[0, pl.ds(0, outer - 1)], send_sem.at[C1])
        arrived(zrecv, send_sem.at[ZZ])
    arrived(pj.at[pl.ds(0, len(gz_peers))], send_sem.at[PJ])


def finish(most, hg_ref, wg_ref, hg_out, wg_out, lines, sem):
    wide = pltpu.make_async_copy(hg_ref, hg_out, sem.at[0])
    wide.start()
    for row in range(most):
        lines[row] = wg_ref[0, 0, row : row + 1, :]
    narrow = pltpu.make_async_copy(lines, wg_out, sem.at[1])
    narrow.start()
    wide.wait()
    narrow.wait()


def shards(hidden_in, norm_gain, normed_grad, key_grad, weight_blocks, block_count):
    outer, inner, quarters = lax.axis_size("gx"), lax.axis_size("gy"), lax.axis_size("gz")
    tokens, rows = hidden_in.shape
    width = key_grad.shape[1]
    most = weight_blocks.shape[2]
    blocks = rows * width // LANES
    pieces = width // LANES
    group_blocks = (blocks + outer - 1) // outer
    slots = round_up(most, 32)
    chips = inner // CORES
    half = chips // 2
    lines = max(half - 1, 1)
    per_group = chips * slots
    padded_outer = round_up(outer, 16)
    span = (group_blocks + pieces - 1) // pieces + 1
    cfg = dict(
        outer=outer, inner=inner, quarters=quarters, chips=chips, slots=slots, most=most,
        group_blocks=group_blocks, blocks=blocks, rows=rows, width=width, pieces=pieces,
        model_width=rows * quarters, padded_outer=padded_outer,
        lane_window=min(rows, round_up(span + LANES - 1, LANES)),
        row_window=min(rows, round_up(span + 7, 8)),
    )
    vmem = pltpu.VMEM
    dma = pltpu.SemaphoreType.DMA
    hg, wg = pl.pallas_call(
        functools.partial(kernel, cfg),
        out_shape=(
            pltpu.VMEM((tokens, rows), BF16),
            pltpu.VMEM(weight_blocks.shape, F32),
        ),
        in_specs=[pl.BlockSpec(memory_space=pltpu.HBM)] * 6,
        out_specs=(pl.BlockSpec(memory_space=pltpu.VMEM), pl.BlockSpec(memory_space=pltpu.VMEM)),
        scratch_shapes=[
            vmem((CORES, tokens, rows), BF16),
            vmem((1, rows), F32),
            vmem((tokens, rows), BF16),
            vmem((CORES * tokens, width), BF16),
            vmem(weight_blocks.shape, BF16),
            vmem(block_count.shape, jnp.int32),
            vmem((CORES * quarters, 8, LANES), F32),
            vmem((CORES * quarters, 8, LANES), F32),
            vmem((CORES, LANES, LANES), F32),
            vmem((CORES * tokens, rows + LANES), BF16),
            vmem((outer, per_group, cfg["lane_window"]), BF16),
            vmem((outer, cfg["row_window"], per_group), BF16),
            vmem((outer, per_group, LANES), jnp.int32),
            vmem((LANES, LANES), F32),
            vmem((8, LANES), F32),
            vmem((chips, outer, slots, LANES), BF16),
            vmem((chips, outer, slots, LANES), F32),
            vmem((chips, outer, slots, LANES), BF16),
            vmem((half, outer, slots, LANES), BF16),
            vmem((lines, outer, slots, LANES), BF16),
            vmem((lines, outer, slots, LANES), BF16),
            vmem((outer, slots, LANES), F32),
            vmem((max(outer - 1, 1), slots, LANES), F32),
            vmem((rows + cfg["row_window"], width), F32),
            vmem((CORES * tokens, rows), F32),
            vmem((tokens, rows), F32),
            dma((6,)), dma((7,)), dma((6,)), dma((17,)), dma((len(BATCHES),)), dma((len(BATCHES),)),
        ],
        compiler_params=pltpu.CompilerParams(
            collective_id=0, has_side_effects=True, vmem_limit_bytes=60_000_000
        ),
        name="key_projection_backward",
    )(hidden_in, norm_gain.reshape(1, rows), normed_grad, key_grad, weight_blocks, block_count)
    hg, wg = pl.pallas_call(
        functools.partial(finish, most),
        out_shape=(
            jax.ShapeDtypeStruct((tokens, rows), BF16),
            jax.ShapeDtypeStruct((most, 1, LANES), F32),
        ),
        in_specs=[pl.BlockSpec(memory_space=pltpu.VMEM)] * 2,
        out_specs=[pl.BlockSpec(memory_space=pltpu.HBM)] * 2,
        scratch_shapes=[vmem((most, 1, LANES), F32), dma((2,))],
        compiler_params=pltpu.CompilerParams(vmem_limit_bytes=2 * 1024 * 1024),
        name="write_results",
    )(hg, wg)
    return hg, wg.reshape(weight_blocks.shape)


def solution(mesh):
    placed = (
        P(("gx", "gy"), "gz"),
        P("gz"),
        P(("gx", "gy"), "gz"),
        P(("gx", "gy"), None),
        P(("gx", "gy"), "gz", None, None),
        P("gz", None),
    )
    return jax.shard_map(
        shards,
        mesh=mesh,
        in_specs=placed,
        out_specs=(P(("gx", "gy"), "gz"), P(("gx", "gy"), "gz", None, None)),
        check_vma=False,
    )
```
